32 devices in a mesh: rep: 1, dp: 32 (over x, y, z, core).
Axes of the slice: x: 2, y: 2, z: 4, core: 2. Of those that a mesh axis runs over, the one named last changes fastest.
Arguments:
- x: bfloat16 [32, 2048, 640], P(('rep', 'dp'))
- dy: bfloat16 [32, 2048, 640], P(('rep', 'dp'))
- w_gate: bfloat16 [2, 640, 2560], P(None, 'dp')
- w_up: bfloat16 [2, 640, 2560], P(None, 'dp')
- w_down: bfloat16 [2, 2560, 640], P(None, 'dp')
Outputs:
- output 1: bfloat16 [32, 2048, 640], P(('rep', 'dp'))
- output 2: bfloat16 [2, 640, 2560], P('rep', 'dp')
- output 3: bfloat16 [2, 640, 2560], P('rep', 'dp')
- output 4: bfloat16 [2, 2560, 640], P('rep', 'dp')
All inputs are finite; a program needn't handle non-finite values.
Results may differ from the reference program's by a relative error of at most 0.018.
Values are sent between devices in bfloat16 or wider.
A program may use at most 2 GiB of HBM per device.

```python
import jax
import jax.numpy as jnp
from jax import lax

SEQUENCES = 32
TOKENS = 2048
D = 640
FF = 2560
LAYERS = 2
NAMES = ("w_gate", "w_up", "w_down")
SHAPES = {"w_gate": (LAYERS, D, FF), "w_up": (LAYERS, D, FF), "w_down": (LAYERS, FF, D)}


def bump(key, n, height):
    away = (jnp.arange(n, dtype=jnp.int32) - jax.random.randint(key, (), 0, n, jnp.int32)) % n
    return jnp.where(away < n // 8, height, 1.0)


def together(key, own, strength):
    shared = jax.random.normal(key, own.shape[1:], jnp.float32)
    return (own + strength * shared) * lax.rsqrt(1 + strength * strength)


def setup_inputs(seed: int = 0, part: int = 0) -> dict:
    kx, kdy, ka, kb, kz, kf, kh, kl, *kw = jax.random.split(jax.random.key(seed), 8 + len(NAMES))
    kx, kdy, ka, kb = (jax.random.fold_in(k, part) for k in (kx, kdy, ka, kb))
    shape = (SEQUENCES, TOKENS, D)
    much_x, much_dy = jax.random.uniform(kz, (2,), jnp.float32, 0.0, 1.0)
    layers = 2.0 ** jax.random.uniform(kl, (LAYERS, 1, 1), jnp.float32, -1.0, 1.0)
    x = together(ka, jax.random.normal(kx, shape, jnp.float32), much_x) * bump(kf, D, 4.0)
    dy = together(kb, jax.random.normal(kdy, shape, jnp.float32), much_dy)
    drawn = {"x": x.astype(jnp.bfloat16), "dy": (dy * (SEQUENCES * TOKENS) ** -0.5).astype(jnp.bfloat16)}
    for key, name in zip(kw, NAMES, strict=True):
        w = jax.random.normal(key, SHAPES[name], jnp.float32) * SHAPES[name][1] ** -0.5
        drawn[name] = (w * {"w_gate": 1.0, "w_up": bump(kh, FF, 4.0), "w_down": layers}[name]).astype(jnp.bfloat16)
    return drawn


def matmul(a, w):
    return jnp.dot(a, w, preferred_element_type=jnp.float32).astype(jnp.bfloat16)


def normed(h):
    wide = h.astype(jnp.float32)
    scale = lax.rsqrt(jnp.mean(wide**2, -1, keepdims=True) + 1e-6)
    return (wide * scale).astype(jnp.bfloat16)


def layer(h, w):
    a = normed(h)
    gate = jnp.dot(a, w["w_gate"], preferred_element_type=jnp.float32)
    up = jnp.dot(a, w["w_up"], preferred_element_type=jnp.float32)
    return h + matmul((jax.nn.silu(gate) * up).astype(jnp.bfloat16), w["w_down"])


def stack(weights, h):
    return lax.scan(lambda h, w: (layer(h, w), None), h, weights)[0]


def reference(x, dy, w_gate, w_up, w_down):
    weights = dict(zip(NAMES, (w_gate, w_up, w_down), strict=True))

    def take(so_far, sequence):
        h, by_y = sequence
        _, back = jax.vjp(stack, weights, h)
        by_weights, by_h = back(by_y)
        return jax.tree.map(lambda total, term: total + term.astype(jnp.float32), so_far, by_weights), by_h

    none_yet = {name: jnp.zeros(w.shape, jnp.float32) for name, w in weights.items()}
    by_weights, by_x = lax.scan(take, none_yet, (x, dy))
    return (by_x, *(by_weights[name].astype(jnp.bfloat16) for name in NAMES))
```

```python
import jax
import jax.numpy as jnp
from jax import lax
from jax.sharding import PartitionSpec as P

LAYERS = 2
BF = jnp.bfloat16
F32 = jnp.float32


def dot(a, b, dims):
    return lax.dot_general(a, b, (dims, ((), ())), preferred_element_type=F32)


NN = ((1,), (0,))
NT = ((1,), (1,))
TN = ((0,), (0,))


GROUP = 4


def exchange(t):
    n = lax.axis_size("dp")
    groups = [[g + i for i in range(GROUP)] for g in range(0, n, GROUP)]
    return lax.all_to_all(t, "dp", 0, 0, axis_index_groups=groups, tiled=True)


def gather(w):
    return lax.all_gather(w, "dp", axis=0, tiled=True)


def scatter(g):
    return lax.psum_scatter(g, "dp", scatter_dimension=0, tiled=True)


def rows_to_blocks(w):
    m, r, f = w.shape
    t = w.reshape(m, r, GROUP, f // GROUP).transpose(2, 0, 1, 3)
    t = exchange(t)
    return t.transpose(1, 0, 2, 3).reshape(m, GROUP * r, f // GROUP)


def blocks_to_rows(b):
    m, r, f = b.shape
    t = b.reshape(m, GROUP, r // GROUP, f).transpose(1, 0, 2, 3)
    t = exchange(t)
    return t.transpose(1, 2, 0, 3).reshape(m, r // GROUP, GROUP * f)


def whole(blocks):
    t = blocks.reshape(-1, GROUP, 80, 640).transpose(0, 2, 1, 3)
    return t.reshape(640, 2560)


def apart(g):
    t = g.reshape(-1, 80, GROUP, 640).transpose(0, 2, 1, 3)
    return t.reshape(-1, 640)


def step(x, dy, wg, wu, wd):
    h = x[0]
    ct = dy[0]
    mine = rows_to_blocks(jnp.concatenate([wg, wu]))
    wgs = [whole(gather(mine[l])) for l in range(LAYERS)]
    wus = [whole(gather(mine[LAYERS + l])) for l in range(LAYERS)]
    wds = [gather(wd[l]) for l in range(LAYERS)]
    saved = []
    for l in range(LAYERS):
        wide = h.astype(F32)
        scale = lax.rsqrt(jnp.mean(wide**2, -1, keepdims=True) + 1e-6)
        a = (wide * scale).astype(BF)
        g = dot(a, wgs[l], NN)
        u = dot(a, wus[l], NN)
        act = (jax.nn.silu(g) * u).astype(BF)
        saved.append((h, scale, a, g, u, act))
        if l < LAYERS - 1:
            h = h + dot(act, wds[l], NN).astype(BF)
    outs = [None] * LAYERS
    for l in reversed(range(LAYERS)):
        h, scale, a, g, u, act = saved[l]
        dact = dot(ct, wds[l], NT).astype(BF).astype(F32)
        s = jax.nn.sigmoid(g)
        du = (dact * (g * s)).astype(BF)
        dg = (dact * u * (s * (1 + g * (1 - s)))).astype(BF)
        dwd = dot(act, ct, TN).astype(BF)
        dwg = dot(a, dg, TN).astype(BF)
        dwu = dot(a, du, TN).astype(BF)
        outs[l] = (scatter(apart(dwg)), scatter(apart(dwu)), scatter(dwd))
        da = (dot(dg, wgs[l], NT) + dot(du, wus[l], NT)).astype(BF).astype(F32)
        wide = h.astype(F32)
        inner = jnp.mean(da * wide, -1, keepdims=True)
        dh = da * scale - wide * (scale * scale * scale * inner)
        ct = ct + dh.astype(BF)
    back = blocks_to_rows(jnp.stack([outs[l][i] for i in range(2) for l in range(LAYERS)]))
    return ct[None], back[:LAYERS], back[LAYERS:], jnp.stack([outs[l][2] for l in range(LAYERS)])


def solution(mesh):
    w = P(None, "dp", None)
    t = P(("rep", "dp"), None, None)
    o = P("rep", "dp", None)
    return jax.shard_map(step, mesh=mesh, in_specs=(t, t, w, w, w), out_specs=(t, o, o, o), check_vma=False)
```

```python
import functools

import jax
import jax.numpy as jnp
from jax import lax
from jax.experimental import pallas as pl
from jax.experimental.pallas import tpu as pltpu
from jax.sharding import PartitionSpec as P

LAYERS = 2
BF = jnp.bfloat16
F32 = jnp.float32
D = 640
FF = 2560
ROWS = 80
CH = 5
LN = 128
FC = 512
GROUP = 4
SLOTS = 4
NN = ((1,), (0,))
NT = ((1,), (1,))


def aligned(i, n):
    return i if isinstance(i, int) else pl.multiple_of(i, n)


def dot(a, b, dims):
    return lax.dot_general(a, b, (dims, ((), ())), preferred_element_type=F32)


def exchange(t):
    n = lax.axis_size("dp")
    groups = [[g + i for i in range(GROUP)] for g in range(0, n, GROUP)]
    return lax.all_to_all(t, "dp", 0, 0, axis_index_groups=groups, tiled=True)


def rows_to_blocks(w):
    m, r, f = w.shape
    t = w.reshape(m, r, GROUP, f // GROUP).transpose(2, 0, 1, 3)
    t = exchange(t)
    return t.transpose(1, 0, 2, 3).reshape(m, GROUP * r, f // GROUP)


def blocks_to_rows(b):
    m, r, f = b.shape
    t = b.reshape(m, GROUP, r // GROUP, f).transpose(1, 0, 2, 3)
    t = exchange(t)
    return t.transpose(1, 2, 0, 3).reshape(m, r // GROUP, GROUP * f)


def kernel(mt, wblk, x_hbm, dy_hbm, out_x, out_gu, out_d,
           W, h, ct, a, aT, ctT, acc, E, R1, R2, R3, R4, S2, S3, S4,
           R1d, R2d, R3d, R4d, S2d, S3d, S4d, lsem, ag_s, ag_r, rs_s, rs_r, rd_s, rd_r):
    T = x_hbm.shape[0]
    tiles = T // mt
    me = lax.axis_index("dp")
    c = me % 2
    z = (me // 2) % 4
    zl = z % 2
    zh = z // 2
    y = (me // 8) % 2
    x = me // 16
    b = me // 2
    nc = 1 - c
    nx = 1 - x
    ny = 1 - y

    def dev(x_, y_, z_, c_):
        return {"dp": ((x_ * 2 + y_) * 4 + z_) * 2 + c_}

    d_core = dev(x, y, z, nc)
    d_x = dev(nx, y, z, c)
    d_y = dev(x, ny, z, c)
    zs = [(z + k) % 4 for k in (1, 2, 3)]
    d_z = [dev(x, y, zz, c) for zz in zs]
    everyone = [d_core, d_x, d_y, *d_z]

    loads = [pltpu.make_async_copy(wblk.at[i], W.at[i, b, c], lsem.at[i]) for i in range(6)]
    loads.append(pltpu.make_async_copy(x_hbm, h, lsem.at[6]))
    loads.append(pltpu.make_async_copy(dy_hbm, ct, lsem.at[7]))
    for i in (2, 0, 1, 5, 3, 4, 6, 7):
        loads[i].start()

    barrier = pltpu.get_barrier_semaphore()
    for d in everyone:
        pl.semaphore_signal(barrier, inc=1, device_id=d, device_id_type=pl.DeviceIdType.MESH)
    pl.semaphore_wait(barrier, len(everyone))

    msgs = [(2, 1, 0, D), (0, 2, 0, 256), (0, 2, 256, 256), (0, 2, 512, 128), (5, 1, 0, D), (3, 2, 0, 256), (3, 2, 256, 384)]
    used = [0]

    def part(msg, first, n):
        m, k, lo, w = msg
        return W.at[pl.ds(m, k), pl.ds(first, n), c, :, pl.ds(lo, w)]

    def push(msg, first, n, d):
        i = used[0]
        used[0] += 1
        ref = part(msg, first, n)
        cp = pltpu.make_async_remote_copy(src_ref=ref, dst_ref=ref, send_sem=ag_s.at[i], recv_sem=ag_r.at[i],
                                          device_id=d, device_id_type=pl.DeviceIdType.MESH)
        return cp

    def start(copies):
        for cp in copies:
            cp.start()

    zc, xy, yx, cc = [], [], [], []
    base = 8 * x + 4 * y
    for g in msgs:
        zc.append([push(g, b, 1, d) for d in d_z])
        xy.append([push(g, base, 2, d_x), push(g, base + 2, 2, d_y)])
        yx.append([push(g, 4 * y, 2, d_y), push(g, 8 + 4 * y, 2, d_y), push(g, 8 * x + 2, 2, d_x), push(g, 8 * x + 6, 2, d_x)])
        cc.append([push(g, base, 4, d_core), push(g, 8 * nx + 4 * y, 2, d_core), push(g, 8 * x + 4 * ny + 2, 2, d_core),
                   push(g, 4 * ny, 2, d_core), push(g, 8 + 4 * ny, 2, d_core), push(g, 8 * nx + 2, 2, d_core), push(g, 8 * nx + 6, 2, d_core)])

    def st_z(i):
        start(zc[i])

    def st_xy(i):
        for cp in zc[i]:
            cp.wait_recv()
        start(xy[i])
        start(cc[i][:1])

    def st_yx(i):
        for cp in xy[i]:
            cp.wait_recv()
        start(yx[i])
        start(cc[i][1:3])

    def st_c(i):
        for cp in yx[i]:
            cp.wait_recv()
        start(cc[i][3:])

    def st_done(i):
        for cp in cc[i]:
            cp.wait_recv()
        for cp in (*zc[i], *xy[i], *yx[i], *cc[i]):
            cp.wait_send()

    def tick(k):
        if 0 <= k < len(msgs):
            st_xy(k)
        if 0 <= k - 1 < len(msgs):
            st_yx(k - 1)
        if 0 <= k - 2 < len(msgs):
            st_c(k - 2)
        if 0 <= k - 3 < len(msgs):
            st_done(k - 3)

    for i in range(6):
        loads[i].wait()
    for i in range(len(msgs)):
        st_z(i)

    def row_tile(i):
        return pl.ds(aligned(i * mt, mt), mt)

    def norm_tile(i, with_ct):
        rows = row_tile(i)
        wide = h[rows, :].astype(F32)
        scale = lax.rsqrt(jnp.mean(wide * wide, -1, keepdims=True) + 1e-6)
        v = (wide * scale).astype(BF)
        a[rows, :] = v
        aT[:, rows] = v.T
        if with_ct:
            ctT[:, rows] = ct[rows, :].T
        acc[rows, :] = jnp.zeros((mt, D), F32)

    def norm_all(with_ct):
        @pl.loop(0, tiles)
        def _(i):
            norm_tile(i, with_ct)

    def lanes(s):
        return pl.ds(aligned(s * LN, LN), LN)

    def columns(m, s):
        cols = []
        for q in range(4):
            cols.append(jnp.concatenate([W[m, 2 * g + q // 2, q % 2, :, lanes(s)] for g in range(8)], axis=0))
        return jnp.concatenate(cols, axis=1)

    def down_place(q, t, s):
        j = 8 * s + t
        k = 8 * q + j // 5
        return k // 2, k % 2, pl.ds(aligned((j % 5) * 16, 16), 16)

    def down_rows(m, s):
        rows = []
        for q in range(4):
            for t in range(8):
                b_, c_, r_ = down_place(q, t, s)
                rows.append(W[m, b_, c_, r_, :])
        return jnp.concatenate(rows, axis=0)

    def forward_chunk(s):
        @pl.loop(0, tiles)
        def _(i):
            rows = row_tile(i)
            v = a[rows, :]
            g = dot(v, columns(0, s), NN)
            u = dot(v, columns(1, s), NN)
            act = (jax.nn.silu(g) * u).astype(BF)
            acc[rows, :] += dot(act, down_rows(2, s), NN)

    def back_tokens(m, s):
        @pl.loop(0, tiles)
        def _(i):
            rows = row_tile(i)
            v = a[rows, :]
            wg = columns(m, s)
            wu = columns(m + 1, s)
            g = dot(v, wg, NN)
            u = dot(v, wu, NN)
            dact = dot(ct[rows, :], down_rows(m + 2, s), NT).astype(BF).astype(F32)
            sg = jax.nn.sigmoid(g)
            si = g * sg
            E[2, rows, :] = (si * u).astype(BF)
            du = (dact * si).astype(BF)
            dg = (dact * u * (sg * (1 + g * (1 - sg)))).astype(BF)
            E[0, rows, :] = dg
            E[1, rows, :] = du
            acc[rows, :] += dot(dg, wg, NT) + dot(du, wu, NT)

    def back_weights(m, s):
        for j in range(2):
            r = dot(aT[...], E[j], NN).astype(BF)
            for q in range(4):
                for g in range(8):
                    W[m + j, 2 * g + q // 2, q % 2, :, lanes(s)] = r[ROWS * g:ROWS * (g + 1), LN * q:LN * (q + 1)]
        r = dot(ctT[...], E[2], NN).astype(BF).T
        for q in range(4):
            for t in range(8):
                b_, c_, r_ = down_place(q, t, s)
                W[m + 2, b_, c_, r_, :] = r[LN * q + 16 * t:LN * q + 16 * (t + 1), :]

    def back_norm(out):
        @pl.loop(0, tiles)
        def _(i):
            rows = row_tile(i)
            wide = h[rows, :].astype(F32)
            scale = lax.rsqrt(jnp.mean(wide * wide, -1, keepdims=True) + 1e-6)
            da = acc[rows, :].astype(BF).astype(F32)
            inner = jnp.mean(da * wide, -1, keepdims=True)
            dh = (da * scale - wide * (scale * scale * scale * inner)).astype(BF)
            out[rows, :] = (ct[rows, :].astype(F32) + dh.astype(F32)).astype(BF)

    def rcopy(src, dst, d, ss, rr):
        return pltpu.make_async_remote_copy(src_ref=src, dst_ref=dst, send_sem=ss, recv_sem=rr,
                                            device_id=d, device_id_type=pl.DeviceIdType.MESH)

    class Reduce:
        def __init__(self, m, n, ln, slot, bufs, ss, rr):
            self.m, self.n, self.ln = m, n, ln
            self.r1, self.r2, self.r3, self.r4, self.s2, self.s3, self.s4 = bufs
            self.slot = slot
            self.c1 = rcopy(W.at[pl.ds(m, n), :, nc, :, ln], self.r1.at[slot], d_core, ss.at[slot, 0], rr.at[slot, 0])
            self.c2 = [rcopy(self.s2.at[k], self.r2.at[slot, k], (d_y, d_x)[k], ss.at[slot, 1 + k], rr.at[slot, 1 + k]) for k in (0, 1)]
            self.c3 = [rcopy(self.s3.at[k], self.r3.at[slot, k], (d_x, d_y)[k], ss.at[slot, 3 + k], rr.at[slot, 3 + k]) for k in (0, 1)]
            self.c4 = [rcopy(self.s4.at[k], self.r4.at[slot, k], d_z[k], ss.at[slot, 5 + k], rr.at[slot, 5 + k]) for k in range(3)]

        def two(self, j, b_):
            return W[self.m + j, b_, c, :, self.ln].astype(F32) + self.r1[self.slot, j, b_].astype(F32)

        def send1(self):
            self.c1.start()

        def send2(self):
            self.c1.wait()
            for j in range(self.n):
                for k in range(2):
                    for l in range(2):
                        self.s2[0, j, 2 * k + l] = self.two(j, 8 * k + 4 * ny + l).astype(BF)
                        self.s2[1, j, 2 * k + l] = self.two(j, 8 * nx + 4 * k + 2 + l).astype(BF)
            for cp in self.c2:
                cp.start()

        def send3(self):
            for cp in self.c2:
                cp.wait()
            for j in range(self.n):
                for l in range(2):
                    v = self.two(j, 8 * nx + 4 * y + l) + self.r2[self.slot, 0, j, 2 * nx + l].astype(F32)
                    self.s3[0, j, l] = v.astype(BF)
                    v = self.two(j, 8 * x + 4 * ny + 2 + l) + self.r2[self.slot, 1, j, 2 * ny + l].astype(F32)
                    self.s3[1, j, l] = v.astype(BF)
            for cp in self.c3:
                cp.start()

        def four(self, j, z_):
            h_ = z_ // 2
            l_ = z_ % 2
            v = self.two(j, 8 * x + 4 * y + z_)
            v += self.r2[self.slot, h_, j, 2 * (x * (1 - h_) + y * h_) + l_].astype(F32)
            return v + self.r3[self.slot, h_, j, l_].astype(F32)

        def send4(self):
            for cp in self.c3:
                cp.wait()
            for j in range(self.n):
                for k in range(3):
                    self.s4[k, j] = self.four(j, zs[k]).astype(BF)
            for cp in self.c4:
                cp.start()

        def finish(self, store):
            for cp in self.c4:
                cp.wait()
            for j in range(self.n):
                v = self.four(j, z)
                for k in range(3):
                    v += self.r4[self.slot, k, j].astype(F32)
                store(j, v.astype(BF))

    gu_bufs = (R1, R2, R3, R4, S2, S3, S4)
    d_bufs = (R1d, R2d, R3d, R4d, S2d, S3d, S4d)

    def layer_of(t):
        return 1 - t // CH

    def gu(t):
        return Reduce(3 * layer_of(t), 2, lanes(t % CH), t % SLOTS, gu_bufs, rs_s, rs_r)

    def dn(t):
        return Reduce(3 * layer_of(t) + 2, 1, pl.ds(0, D), 0, d_bufs, rd_s, rd_r)

    def store_gu(t):
        l = layer_of(t)

        def f(j, v):
            out_gu[l, j, :, lanes(t % CH)] = v
        return f

    def store_d(t):
        l = layer_of(t)

        def f(j, v):
            out_d[l] = v
        return f

    def both(t, lo, f):
        @pl.when((t >= 0) & (t < 2 * CH))
        def _():
            f(gu(t), store_gu(t))

            @pl.when(t % CH == CH - 1)
            def _():
                f(dn(t), store_d(t))

    tick(0)
    tick(1)
    loads[6].wait()
    loads[7].wait()
    norm_all(True)
    tick(2)
    tick(3)
    tick(4)

    @pl.loop(0, 2)
    def _(s):
        forward_chunk(s)

    tick(5)

    @pl.loop(2, 4)
    def _(s):
        forward_chunk(s)

    tick(6)
    forward_chunk(4)

    @pl.loop(0, tiles)
    def _(i):
        rows = row_tile(i)
        h[rows, :] = (h[rows, :].astype(F32) + acc[rows, :].astype(BF).astype(F32)).astype(BF)

    norm_all(False)
    st_yx(6)
    st_c(5)
    st_done(4)
    st_done(5)

    @pl.loop(0, 2 * CH + 2)
    def _(t):
        m = 3 * (1 - t // CH)
        s = t % CH

        @pl.when(t == 1)
        def _():
            st_c(6)

        @pl.when(t == 2)
        def _():
            st_done(6)

        @pl.when(t < 2 * CH)
        def _():
            back_tokens(m, s)

        both(t - 1, 0, lambda r, st: r.send2())
        both(t - 2, 0, lambda r, st: r.send4())

        @pl.when(t < 2 * CH)
        def _():
            back_weights(m, s)

        both(t, 0, lambda r, st: r.send1())
        both(t - 1, 0, lambda r, st: r.send3())
        both(t - 2, 0, lambda r, st: r.finish(st))

        @pl.when(t == CH - 1)
        def _():
            back_norm(ct)
            again = pltpu.make_async_copy(x_hbm, h, lsem.at[6])
            again.start()
            again.wait()
            norm_all(True)

        @pl.when(t == 2 * CH - 1)
        def _():
            back_norm(out_x)


def step(x, dy, wg, wu, wd):
    t = x.shape[1]
    mt = min(512, t)
    mine = rows_to_blocks(jnp.concatenate([wg, wu]))
    wblk = jnp.stack([mine[0], mine[2], wd[0], mine[1], mine[3], wd[1]])
    ag = 16 * 7
    dma = pltpu.SemaphoreType.DMA

    def v(*shape, dtype=BF):
        return pltpu.VMEM(shape, dtype)

    def rs_bufs(slots, n, w):
        r = [v(slots, n, 16, ROWS, w), v(slots, 2, n, 4, ROWS, w), v(slots, 2, n, 2, ROWS, w), v(slots, 3, n, ROWS, w)]
        return r, [v(2, n, 4, ROWS, w), v(2, n, 2, ROWS, w), v(3, n, ROWS, w)]

    gr, gs = rs_bufs(SLOTS, 2, LN)
    dr, ds_ = rs_bufs(1, 1, D)
    vm = pl.BlockSpec(memory_space=pltpu.VMEM)
    hbm = pl.BlockSpec(memory_space=pl.ANY)
    flops = 22 * 2 * t * D * FF
    out_x, out_gu, out_d = pl.pallas_call(
        functools.partial(kernel, mt),
        out_shape=(jax.ShapeDtypeStruct((t, D), BF), jax.ShapeDtypeStruct((LAYERS, 2, ROWS, D), BF), jax.ShapeDtypeStruct((LAYERS, ROWS, D), BF)),
        in_specs=[hbm, hbm, hbm],
        out_specs=(vm, vm, vm),
        scratch_shapes=[
            v(6, 16, 2, ROWS, D), v(t, D), v(t, D), v(t, D), v(D, t), v(D, t), v(t, D, dtype=F32), v(3, t, FC),
            *gr, *gs, *dr, *ds_,
            dma((8,)), dma((ag,)), dma((ag,)), dma((SLOTS, 8)), dma((SLOTS, 8)), dma((1, 8)), dma((1, 8)),
        ],
        compiler_params=pltpu.CompilerParams(collective_id=0, has_side_effects=True, vmem_limit_bytes=67043328),
        cost_estimate=pl.CostEstimate(flops=flops, bytes_accessed=40_000_000, transcendentals=0),
        name="stack",
    )(wblk, x[0], dy[0])
    back = blocks_to_rows(out_gu.transpose(1, 0, 2, 3).reshape(2 * LAYERS, ROWS, D))
    return out_x[None], back[:LAYERS], back[LAYERS:], out_d


def solution(mesh):
    w = P(None, "dp", None)
    t = P(("rep", "dp"), None, None)
    o = P("rep", "dp", None)
    return jax.shard_map(step, mesh=mesh, in_specs=(t, t, w, w, w), out_specs=(t, o, o, o), check_vma=False)
```

```python
import jax
import jax.numpy as jnp
from jax import lax
from jax.experimental import pallas as pl
from jax.experimental.pallas import tpu as pltpu
from jax.sharding import PartitionSpec as P

LAYERS = 2
BF = jnp.bfloat16
F32 = jnp.float32
D = 640
FF = 2560
ROWS = 80
CH = 5
LN = 128
FC = 512
GROUP = 4
PIECE = 20
PAD = 32
TILES = 4
SLOTS = 4
NN = ((1,), (0,))
NT = ((1,), (1,))


def aligned(i, n):
    return i if isinstance(i, int) else pl.multiple_of(i, n)


def dot(a, b, dims):
    return lax.dot_general(a, b, (dims, ((), ())), preferred_element_type=F32)


def kernel(wg, wu, wd_hbm, x_hbm, dy_hbm, out_x, out_g, out_u, out_d, gu_hbm, act_hbm,
           W, h, ct, a, aT, ctT, acc, E, G, TD, R1, R2, R3, R4, S2, S3, S4,
           R1d, R2d, R3d, R4d, XS, XR, OB,
           lsem, gsem, esem, ag_s, ag_r, rs_s, rs_r, rd_s, rd_r, xs_s, xs_r, ys_s, ys_r):
    T = x_hbm.shape[0]
    tiles = TILES
    mt = T // tiles
    me = lax.axis_index("dp")
    c = me % 2
    z = (me // 2) % 4
    zl = z % 2
    y = (me // 8) % 2
    x = me // 16
    b = me // 2
    q = me % GROUP
    nc = 1 - c
    nx = 1 - x
    ny = 1 - y

    def dev(x_, y_, z_, c_):
        return {"dp": ((x_ * 2 + y_) * 4 + z_) * 2 + c_}

    d_core = dev(x, y, z, nc)
    d_x = dev(nx, y, z, c)
    d_y = dev(x, ny, z, c)
    zs = [(z + k) % 4 for k in (1, 2, 3)]
    d_z = [dev(x, y, zz, c) for zz in zs]
    qs = [(q + k) % GROUP for k in (1, 2, 3)]
    d_q = [{"dp": me - q + qq} for qq in qs]
    everyone = [d_core, d_x, d_y, *d_z, dev(x, y, z + 1 - 2 * zl, nc)]

    def rcopy(src, dst, d, ss, rr):
        return pltpu.make_async_remote_copy(src_ref=src, dst_ref=dst, send_sem=ss, recv_sem=rr,
                                            device_id=d, device_id_type=pl.DeviceIdType.MESH)

    loads = [pltpu.make_async_copy(wd_hbm.at[l], W.at[3 * l + 2, b, c], lsem.at[l]) for l in range(LAYERS)]
    loads.append(pltpu.make_async_copy(x_hbm, h, lsem.at[2]))
    loads.append(pltpu.make_async_copy(dy_hbm, ct, lsem.at[3]))
    for cp in loads:
        cp.start()
    for qq in range(GROUP):
        for l in range(LAYERS):
            for j, w in enumerate((wg, wu)):
                XS[qq, 2 * l + j] = jnp.zeros((PAD, D), BF)
                XS[qq, 2 * l + j, 0:PIECE, :] = w[l, :, D * qq:D * (qq + 1)]

    barrier = pltpu.get_barrier_semaphore()
    for d in everyone:
        pl.semaphore_signal(barrier, inc=1, device_id=d, device_id_type=pl.DeviceIdType.MESH)
    pl.semaphore_wait(barrier, len(everyone))

    xc = [rcopy(XS.at[qs[k]], XR.at[q], d_q[k], xs_s.at[k], xs_r.at[k]) for k in range(3)]
    for cp in xc:
        cp.start()
    row = lax.broadcasted_iota(jnp.int32, (ROWS, GROUP * PAD), 0)
    col = lax.broadcasted_iota(jnp.int32, (ROWS, GROUP * PAD), 1)
    inside = col % PAD
    pick = jnp.where((inside < PIECE) & (inside + PIECE * (col // PAD) == row), 1.0, 0.0).astype(BF)
    row = lax.broadcasted_iota(jnp.int32, (GROUP * PAD, ROWS), 1)
    col = lax.broadcasted_iota(jnp.int32, (GROUP * PAD, ROWS), 0)
    inside = col % PAD
    place = jnp.where((inside < PIECE) & (inside + PIECE * (col // PAD) == row), 1.0, 0.0).astype(BF)

    msgs = [(2, 1, 0, 128), (2, 1, 128, 512), (0, 2, 0, 256), (0, 2, 256, 256), (0, 2, 512, 128),
            (3, 2, 0, 256), (3, 2, 256, 256), (3, 2, 512, 128), (5, 1, 0, 384), (5, 1, 384, 256)]
    used = [0]

    def part(msg, first, n):
        m, k, lo, w = msg
        return W.at[pl.ds(m, k), pl.ds(first, n), c, :, pl.ds(lo, w)]

    def push(msg, first, n, d):
        i = used[0]
        used[0] += 1
        ref = part(msg, first, n)
        return rcopy(ref, ref, d, ag_s.at[i], ag_r.at[i])

    def start(copies):
        for cp in copies:
            cp.start()

    zc, xy, yx, cc = [], [], [], []
    base = 8 * x + 4 * y
    for g in msgs:
        zc.append([push(g, b, 1, d) for d in d_z])
        xy.append([push(g, base, 2, d_x), push(g, base + 2, 2, d_y)])
        yx.append([push(g, 4 * y, 2, d_y), push(g, 8 + 4 * y, 2, d_y), push(g, 8 * x + 2, 2, d_x), push(g, 8 * x + 6, 2, d_x)])
        cc.append([push(g, base, 4, d_core), push(g, 8 * nx + 4 * y, 2, d_core), push(g, 8 * x + 4 * ny + 2, 2, d_core),
                   push(g, 4 * ny, 2, d_core), push(g, 8 + 4 * ny, 2, d_core), push(g, 8 * nx + 2, 2, d_core), push(g, 8 * nx + 6, 2, d_core)])

    def st_z(i):
        start(zc[i])

    def st_xy(i):
        for cp in zc[i]:
            cp.wait_recv()
        start(xy[i])
        start(cc[i][:1])

    def st_yx(i):
        for cp in xy[i]:
            cp.wait_recv()
        start(yx[i])
        start(cc[i][1:3])

    def st_c(i):
        for cp in yx[i]:
            cp.wait_recv()
        start(cc[i][3:])

    def st_done(i):
        for cp in cc[i]:
            cp.wait_recv()
        for cp in (*zc[i], *xy[i], *yx[i], *cc[i]):
            cp.wait_send()

    def tick(k):
        if 0 <= k < len(msgs):
            st_xy(k)
        if 0 <= k - 1 < len(msgs):
            st_yx(k - 1)
        if 0 <= k - 2 < len(msgs):
            st_c(k - 2)
        if 0 <= k - 3 < len(msgs):
            st_done(k - 3)

    loads[0].wait()
    loads[1].wait()
    st_z(0)
    st_z(1)
    XR[q] = XS[q]
    for cp in xc:
        cp.wait()
    for l in range(LAYERS):
        for j in range(2):
            pieces = XR[:, 2 * l + j].reshape(GROUP * PAD, D)
            W[3 * l + j, b, c] = dot(pick, pieces, NN).astype(BF)
    for i in range(2, len(msgs)):
        st_z(i)

    def row_tile(i):
        return pl.ds(aligned(i * mt, mt), mt)

    def norm_all(with_a, with_t):
        @pl.loop(0, tiles)
        def _(i):
            rows = row_tile(i)
            wide = h[rows, :].astype(F32)
            scale = lax.rsqrt(jnp.mean(wide * wide, -1, keepdims=True) + 1e-6)
            v = (wide * scale).astype(BF)
            if with_a:
                a[rows, :] = v
            if with_t:
                aT[:, rows] = v.T
                ctT[:, rows] = ct[rows, :].T
            acc[rows, :] = jnp.zeros((mt, D), F32)

    def lanes(s):
        return pl.ds(aligned(s * LN, LN), LN)

    def columns(m, s):
        cols = []
        for q in range(4):
            cols.append(jnp.concatenate([W[m, 2 * g + q // 2, q % 2, :, lanes(s)] for g in range(8)], axis=0))
        return jnp.concatenate(cols, axis=1)

    def down_place(q, t, s):
        j = 8 * s + t
        k = 8 * q + j // 5
        return k // 2, k % 2, pl.ds(aligned((j % 5) * 16, 16), 16)

    def down_rows(m, s):
        rows = []
        for q in range(4):
            for t in range(8):
                b_, c_, r_ = down_place(q, t, s)
                rows.append(W[m, b_, c_, r_, :])
        return jnp.concatenate(rows, axis=0)

    def keep(l, n):
        return pltpu.make_async_copy(G.at[n % 2], gu_hbm.at[l, n], gsem.at[n % 2])

    def fetch(n):
        return pltpu.make_async_copy(gu_hbm.at[1 - n // (CH * tiles), n % (CH * tiles)], G.at[n % 2], gsem.at[n % 2])

    def keep_act(s):
        return pltpu.make_async_copy(E.at[s % 2], act_hbm.at[s], esem.at[s % 2])

    def fetch_act(s):
        return pltpu.make_async_copy(act_hbm.at[s], E.at[s % 2], esem.at[s % 2])

    def forward_tile(l, s, i, n):
        rows = row_tile(i)

        @pl.when(n >= 2)
        def _():
            keep(l, n - 2).wait()

        v = a[rows, :]
        g = dot(v, columns(3 * l, s), NN)
        u = dot(v, columns(3 * l + 1, s), NN)
        G[n % 2, 0] = g
        G[n % 2, 1] = u
        keep(l, n).start()
        act = (jax.nn.silu(g) * u).astype(BF)
        E[s % 2, rows, :] = act
        return rows, act

    def down_grad(k):
        r = dot(ctT[...], E[k % 2], NN).astype(BF).T
        for qq in range(4):
            for t in range(8):
                b_, c_, r_ = down_place(qq, t, k)
                TD[0, b_, c_, r_, :] = r[LN * qq + 16 * t:LN * qq + 16 * (t + 1), :]

    def back_tile(m, s, i, n):
        rows = row_tile(i)
        fetch(n).wait()

        @pl.when(n + 1 < 2 * CH * tiles)
        def _():
            fetch(n + 1).start()

        wgc = columns(m, s)
        wuc = columns(m + 1, s)
        dact = dot(ct[rows, :], down_rows(m + 2, s), NT).astype(BF).astype(F32)
        g = G[n % 2, 0]
        u = G[n % 2, 1]
        sg = jax.nn.sigmoid(g)
        du = (dact * (g * sg)).astype(BF)
        dg = (dact * u * (sg * (1 + g * (1 - sg)))).astype(BF)
        E[0, rows, :] = dg
        E[1, rows, :] = du
        acc[rows, :] += dot(dg, wgc, NT) + dot(du, wuc, NT)

    def back_weights(m, s):
        for j in range(2):
            r = dot(aT[...], E[j], NN).astype(BF)
            for qq in range(4):
                for g in range(8):
                    W[m + j, 2 * g + qq // 2, qq % 2, :, lanes(s)] = r[ROWS * g:ROWS * (g + 1), LN * qq:LN * (qq + 1)]

    def back_norm(out):
        @pl.loop(0, tiles)
        def _(i):
            rows = row_tile(i)
            wide = h[rows, :].astype(F32)
            scale = lax.rsqrt(jnp.mean(wide * wide, -1, keepdims=True) + 1e-6)
            da = acc[rows, :].astype(BF).astype(F32)
            inner = jnp.mean(da * wide, -1, keepdims=True)
            dh = (da * scale - wide * (scale * scale * scale * inner)).astype(BF)
            out[rows, :] = (ct[rows, :].astype(F32) + dh.astype(F32)).astype(BF)

    class Reduce:
        def __init__(self, term, m, n, ln, slot, bufs, ss, rr):
            self.term, self.m, self.n, self.ln = term, m, n, ln
            self.r1, self.r2, self.r3, self.r4, self.s2, self.s3, self.s4 = bufs
            self.slot = slot
            self.c1 = rcopy(term.at[pl.ds(m, n), :, nc, :, ln], self.r1.at[slot], d_core, ss.at[slot, 0], rr.at[slot, 0])
            self.c2 = [rcopy(self.s2[k], self.r2.at[slot, k], (d_y, d_x)[k], ss.at[slot, 1 + k], rr.at[slot, 1 + k]) for k in (0, 1)]
            self.c3 = [rcopy(self.s3[k], self.r3.at[slot, k], (d_x, d_y)[k], ss.at[slot, 3 + k], rr.at[slot, 3 + k]) for k in (0, 1)]
            self.c4 = [rcopy(self.s4[k], self.r4.at[slot, k], d_z[k], ss.at[slot, 5 + k], rr.at[slot, 5 + k]) for k in range(3)]

        def two(self, j, b_):
            return self.term[self.m + j, b_, c, :, self.ln].astype(F32) + self.r1[self.slot, j, b_].astype(F32)

        def send1(self):
            self.c1.start()

        def send2(self):
            self.c1.wait()
            for j in range(self.n):
                for k in range(2):
                    for l in range(2):
                        self.s2[0][j, 2 * k + l] = self.two(j, 8 * k + 4 * ny + l).astype(BF)
                        self.s2[1][j, 2 * k + l] = self.two(j, 8 * nx + 4 * k + 2 + l).astype(BF)
            for cp in self.c2:
                cp.start()

        def send3(self):
            for cp in self.c2:
                cp.wait()
            for j in range(self.n):
                for l in range(2):
                    v = self.two(j, 8 * nx + 4 * y + l) + self.r2[self.slot, 0, j, 2 * nx + l].astype(F32)
                    self.s3[0][j, l] = v.astype(BF)
                    v = self.two(j, 8 * x + 4 * ny + 2 + l) + self.r2[self.slot, 1, j, 2 * ny + l].astype(F32)
                    self.s3[1][j, l] = v.astype(BF)
            for cp in self.c3:
                cp.start()

        def four(self, j, z_):
            h_ = z_ // 2
            l_ = z_ % 2
            v = self.two(j, 8 * x + 4 * y + z_)
            v += self.r2[self.slot, h_, j, 2 * (x * (1 - h_) + y * h_) + l_].astype(F32)
            return v + self.r3[self.slot, h_, j, l_].astype(F32)

        def send4(self):
            for cp in self.c3:
                cp.wait()
            for j in range(self.n):
                for k in range(3):
                    self.s4[k][j] = self.four(j, zs[k]).astype(BF)
            for cp in self.c4:
                cp.start()

        def finish(self, store):
            for cp in self.c4:
                cp.wait()
            for j in range(self.n):
                v = self.four(j, z)
                for k in range(3):
                    v += self.r4[self.slot, k, j].astype(F32)
                store(j, v.astype(BF))

    gu_bufs = (R1, R2, R3, R4, [S2.at[k] for k in range(2)], [S3.at[k] for k in range(2)], [S4.at[k] for k in range(3)])
    d_bufs = (R1d, R2d, R3d, R4d, [TD.at[pl.ds(0, 1), pl.ds(4 * k, 4), nc] for k in range(2)],
              [TD.at[pl.ds(0, 1), pl.ds(8 + 2 * k, 2), nc] for k in range(2)], [TD.at[pl.ds(0, 1), 12 + k, nc] for k in range(3)])

    def layer_of(t):
        return 1 - t // CH

    def gu(t):
        return Reduce(W, 3 * layer_of(t), 2, lanes(t % CH), t % SLOTS, gu_bufs, rs_s, rs_r)

    down = Reduce(TD, 0, 1, pl.ds(0, D), 0, d_bufs, rd_s, rd_r)

    def store_gu(t):
        l = layer_of(t)

        def f(j, v):
            OB[l, j, :, lanes(t % CH)] = v
        return f

    def store_d(t):
        l = 1 - t // CH

        def f(j, v):
            out_d[l] = v
        return f

    def chunk(t, f):
        @pl.when((t >= 0) & (t < 2 * CH))
        def _():
            f(gu(t))

    def yc(l):
        return [rcopy(XS.at[qs[k], pl.ds(2 * l, 2)], XR.at[q, pl.ds(2 * l, 2)], d_q[k], ys_s.at[l, k], ys_r.at[l, k]) for k in range(3)]

    def hand_back(l):
        for j in range(2):
            r = dot(place, OB[l, j], NN).astype(BF)
            for qq in range(GROUP):
                XS[qq, 2 * l + j] = r[PAD * qq:PAD * (qq + 1), :]
        for cp in yc(l):
            cp.start()

    def take_back(l):
        XR[q, pl.ds(2 * l, 2)] = XS[q, pl.ds(2 * l, 2)]
        for cp in yc(l):
            cp.wait()
        for j, o in enumerate((out_g, out_u)):
            for qq in range(GROUP):
                o[l, :, D * qq:D * (qq + 1)] = XR[qq, 2 * l + j, 0:PIECE, :]

    tick(0)
    tick(1)
    loads[2].wait()
    norm_all(True, False)
    tick(2)
    tick(3)
    tick(4)
    tick(5)

    def at(n, k, f):
        @pl.when(n == k)
        def _():
            f()

    def forward_hooks(n):
        def f4():
            st_xy(6)
            st_yx(5)

        def f8():
            st_c(4)
            st_done(3)

        def f12():
            st_xy(7)
            st_yx(6)

        def f16():
            st_c(5)
            st_done(4)

        def f18():
            st_xy(8)
            st_yx(7)

        for k, f in ((4, f4), (8, f8), (12, f12), (16, f16), (18, f18)):
            at(n, k, f)

    @pl.loop(0, CH * tiles)
    def _(n):
        forward_hooks(n)
        s = n // tiles
        i = n % tiles

        @pl.when((i == 0) & (s >= 2))
        def _():
            keep_act(s - 2).wait()

        rows, act = forward_tile(0, s, i, n)

        @pl.when(i == tiles - 1)
        def _():
            keep_act(s).start()

        acc[rows, :] += dot(act, down_rows(2, s), NN)

    @pl.loop(0, tiles)
    def _(i):
        rows = row_tile(i)
        h[rows, :] = (h[rows, :].astype(F32) + acc[rows, :].astype(BF).astype(F32)).astype(BF)

    st_c(6)
    loads[3].wait()
    norm_all(True, True)
    for n in (CH * tiles - 2, CH * tiles - 1):
        keep(0, n).wait()
    for s in (CH - 2, CH - 1):
        keep_act(s).wait()
    st_done(5)

    @pl.loop(0, CH)
    def _(s):
        def f1():
            st_xy(9)
            st_yx(8)
            st_c(7)

        def f2():
            st_done(6)

        def f3():
            st_yx(9)
            st_c(8)

        def f4():
            st_done(7)

        for k, f in ((1, f1), (2, f2), (3, f3), (4, f4)):
            at(s, k, f)

        @pl.loop(0, tiles)
        def _(i):
            forward_tile(1, s, i, s * tiles + i)

        down_grad(s)

    down.send1()
    for n in (CH * tiles - 2, CH * tiles - 1):
        keep(1, n).wait()
    fetch(0).start()
    st_c(9)
    st_done(8)
    st_done(9)

    @pl.loop(0, 2 * CH + 2)
    def _(t):
        m = 3 * (1 - t // CH)
        s = t % CH
        compute = t < 2 * CH

        @pl.when(compute)
        def _():
            @pl.loop(0, tiles)
            def _(i):
                at(i, 2, lambda: chunk(t - 1, lambda r: r.send2()))
                at(i, 3, lambda: chunk(t - 2, lambda r: r.send4()))
                back_tile(m, s, i, t * tiles + i)

            at(s, 0, lambda: down.send2())
            at(s, 1, lambda: down.send3())
            at(s, 2, lambda: down.send4())
            at(s, 3, lambda: down.finish(store_d(t)))
            back_weights(m, s)

        @pl.when(t >= 2 * CH)
        def _():
            chunk(t - 1, lambda r: r.send2())
            chunk(t - 2, lambda r: r.send4())

        chunk(t, lambda r: r.send1())
        chunk(t - 1, lambda r: r.send3())
        chunk(t - 2, lambda r: r.finish(store_gu(t - 2)))

        @pl.when(t == CH - 1)
        def _():
            back_norm(ct)
            again = pltpu.make_async_copy(x_hbm, h, lsem.at[2])
            again.start()
            fetch_act(0).start()
            fetch_act(1).start()
            again.wait()
            norm_all(False, True)

            @pl.loop(0, CH)
            def _(k):
                fetch_act(k).wait()
                down_grad(k)

                @pl.when(k + 2 < CH)
                def _():
                    fetch_act(k + 2).start()

            down.send1()

        @pl.when(t == CH + 1)
        def _():
            hand_back(1)

        @pl.when(t == 2 * CH - 1)
        def _():
            back_norm(ct)
            pltpu.make_async_copy(ct, out_x, lsem.at[3]).start()

    hand_back(0)
    take_back(1)
    take_back(0)
    pltpu.make_async_copy(ct, out_x, lsem.at[3]).wait()


def step(x, dy, wg, wu, wd):
    t = x.shape[1]
    mt = t // TILES
    ag = 16 * 10
    dma = pltpu.SemaphoreType.DMA

    def v(*shape, dtype=BF):
        return pltpu.VMEM(shape, dtype)

    def rs_bufs(slots, n, w):
        r = [v(slots, n, 16, ROWS, w), v(slots, 2, n, 4, ROWS, w), v(slots, 2, n, 2, ROWS, w), v(slots, 3, n, ROWS, w)]
        return r, [v(2, n, 4, ROWS, w), v(2, n, 2, ROWS, w), v(3, n, ROWS, w)]

    gr, gs = rs_bufs(SLOTS, 2, LN)
    dr, _ = rs_bufs(1, 1, D)
    vm = pl.BlockSpec(memory_space=pltpu.VMEM)
    hbm = pl.BlockSpec(memory_space=pl.ANY)
    flops = 17 * 2 * t * D * FF

    def out(*shape, dtype=BF):
        return jax.ShapeDtypeStruct(shape, dtype)

    out_x, out_g, out_u, out_d, _, _ = pl.pallas_call(
        kernel,
        out_shape=(out(t, D), out(LAYERS, PIECE, FF), out(LAYERS, PIECE, FF), out(LAYERS, ROWS, D),
                   out(LAYERS, CH * TILES, 2, mt, FC, dtype=F32), out(CH, t, FC)),
        in_specs=[vm, vm, hbm, hbm, hbm],
        out_specs=(hbm, vm, vm, vm, hbm, hbm),
        scratch_shapes=[
            v(6, 16, 2, ROWS, D), v(t, D), v(t, D), v(t, D), v(D, t), v(D, t), v(t, D, dtype=F32), v(2, t, FC),
            v(2, 2, mt, FC, dtype=F32), v(1, 16, 2, ROWS, D),
            *gr, *gs, *dr,
            v(GROUP, 4, PAD, D), v(GROUP, 4, PAD, D), v(LAYERS, 2, ROWS, D),
            dma((4,)), dma((2,)), dma((2,)), dma((ag,)), dma((ag,)), dma((SLOTS, 8)), dma((SLOTS, 8)), dma((1, 8)), dma((1, 8)),
            dma((3,)), dma((3,)), dma((LAYERS, 3)), dma((LAYERS, 3)),
        ],
        compiler_params=pltpu.CompilerParams(collective_id=0, has_side_effects=True, vmem_limit_bytes=67043328),
        cost_estimate=pl.CostEstimate(flops=flops, bytes_accessed=180_000_000, transcendentals=0),
        name="stack",
    )(wg, wu, wd, x[0], dy[0])
    return out_x[None], out_g, out_u, out_d


def solution(mesh):
    w = P(None, "dp", None)
    t = P(("rep", "dp"), None, None)
    o = P("rep", "dp", None)
    return jax.shard_map(step, mesh=mesh, in_specs=(t, t, w, w, w), out_specs=(t, o, o, o), check_vma=False)
```

```python
import jax
import jax.numpy as jnp
from jax import lax
from jax.experimental import pallas as pl
from jax.experimental.pallas import tpu as pltpu
from jax.sharding import PartitionSpec as P

LAYERS = 2
BF = jnp.bfloat16
F32 = jnp.float32
D = 640
FF = 2560
ROWS = 80
CH = 5
LN = 128
FC = 512
GROUP = 4
PIECE = 20
PAD = 32
TILES = 4
SLOTS = 4
NN = ((1,), (0,))
NT = ((1,), (1,))


def aligned(i, n):
    return i if isinstance(i, int) else pl.multiple_of(i, n)


def dot(a, b, dims):
    return lax.dot_general(a, b, (dims, ((), ())), preferred_element_type=F32)


def kernel(wg, wu, wd_hbm, x_hbm, dy_hbm, out_x, out_g, out_u, out_d, gu_hbm, act_hbm,
           W, h, ct, a, aT, ctT, acc, E, G, TD, R1, R2, R3, R4, S2, S3, S4,
           R1d, R2d, R3d, R4d, XS, XR, OB,
           lsem, gsem, esem, ag_s, ag_r, rs_s, rs_r, rd_s, rd_r, xs_s, xs_r, ys_s, ys_r):
    T = x_hbm.shape[0]
    tiles = TILES
    mt = T // tiles
    me = lax.axis_index("dp")
    c = me % 2
    z = (me // 2) % 4
    zl = z % 2
    y = (me // 8) % 2
    x = me // 16
    b = me // 2
    q = me % GROUP
    nc = 1 - c
    nx = 1 - x
    ny = 1 - y

    def dev(x_, y_, z_, c_):
        return {"dp": ((x_ * 2 + y_) * 4 + z_) * 2 + c_}

    d_core = dev(x, y, z, nc)
    d_x = dev(nx, y, z, c)
    d_y = dev(x, ny, z, c)
    zs = [(z + k) % 4 for k in (1, 2, 3)]
    d_z = [dev(x, y, zz, c) for zz in zs]
    qs = [(q + k) % GROUP for k in (1, 2, 3)]
    d_q = [{"dp": me - q + qq} for qq in qs]
    everyone = [d_core, d_x, d_y, *d_z, dev(x, y, z + 1 - 2 * zl, nc)]

    def rcopy(src, dst, d, ss, rr):
        return pltpu.make_async_remote_copy(src_ref=src, dst_ref=dst, send_sem=ss, recv_sem=rr,
                                            device_id=d, device_id_type=pl.DeviceIdType.MESH)

    loads = [pltpu.make_async_copy(wd_hbm.at[l], W.at[3 * l + 2, b, c], lsem.at[l]) for l in range(LAYERS)]
    loads.append(pltpu.make_async_copy(x_hbm, h, lsem.at[2]))
    loads.append(pltpu.make_async_copy(dy_hbm, ct, lsem.at[3]))
    for cp in loads:
        cp.start()
    for qq in range(GROUP):
        for l in range(LAYERS):
            for j, w in enumerate((wg, wu)):
                XS[qq, 2 * l + j] = jnp.zeros((PAD, D), BF)
                XS[qq, 2 * l + j, 0:PIECE, :] = w[l, :, D * qq:D * (qq + 1)]

    loads[0].wait()
    loads[1].wait()
    barrier = pltpu.get_barrier_semaphore()
    for d in everyone:
        pl.semaphore_signal(barrier, inc=1, device_id=d, device_id_type=pl.DeviceIdType.MESH)
    pl.semaphore_wait(barrier, len(everyone))

    xc = [[rcopy(XS.at[qs[k], pl.ds(2 * l, 2)], XR.at[q, pl.ds(2 * l, 2)], d_q[k], xs_s.at[l, k], xs_r.at[l, k]) for k in range(3)]
          for l in range(LAYERS)]
    row = lax.broadcasted_iota(jnp.int32, (ROWS, GROUP * PAD), 0)
    col = lax.broadcasted_iota(jnp.int32, (ROWS, GROUP * PAD), 1)
    inside = col % PAD
    pick = jnp.where((inside < PIECE) & (inside + PIECE * (col // PAD) == row), 1.0, 0.0).astype(BF)
    row = lax.broadcasted_iota(jnp.int32, (GROUP * PAD, ROWS), 1)
    col = lax.broadcasted_iota(jnp.int32, (GROUP * PAD, ROWS), 0)
    inside = col % PAD
    place = jnp.where((inside < PIECE) & (inside + PIECE * (col // PAD) == row), 1.0, 0.0).astype(BF)

    msgs = [(2, 1, 0, 128), (2, 1, 128, 512), (0, 2, 0, 256), (0, 2, 256, 256), (0, 2, 512, 128),
            (3, 2, 0, 256), (3, 2, 256, 256), (3, 2, 512, 128), (5, 1, 0, 384), (5, 1, 384, 256)]
    used = [0]

    def part(msg, first, n):
        m, k, lo, w = msg
        return W.at[pl.ds(m, k), pl.ds(first, n), c, :, pl.ds(lo, w)]

    def push(msg, first, n, d):
        i = used[0]
        used[0] += 1
        ref = part(msg, first, n)
        return rcopy(ref, ref, d, ag_s.at[i], ag_r.at[i])

    def start(copies):
        for cp in copies:
            cp.start()

    zc, xy, yx, cc = [], [], [], []
    base = 8 * x + 4 * y
    for g in msgs:
        zc.append([push(g, b, 1, d) for d in d_z])
        xy.append([push(g, base, 2, d_x), push(g, base + 2, 2, d_y)])
        yx.append([push(g, 4 * y, 2, d_y), push(g, 8 + 4 * y, 2, d_y), push(g, 8 * x + 2, 2, d_x), push(g, 8 * x + 6, 2, d_x)])
        cc.append([push(g, base, 4, d_core), push(g, 8 * nx + 4 * y, 2, d_core), push(g, 8 * x + 4 * ny + 2, 2, d_core),
                   push(g, 4 * ny, 2, d_core), push(g, 8 + 4 * ny, 2, d_core), push(g, 8 * nx + 2, 2, d_core), push(g, 8 * nx + 6, 2, d_core)])

    def st_z(i):
        start(zc[i])

    def st_xy(i):
        for cp in zc[i]:
            cp.wait_recv()
        start(xy[i])
        start(cc[i][:1])

    def st_yx(i):
        for cp in xy[i]:
            cp.wait_recv()
        start(yx[i])
        start(cc[i][1:3])

    def st_c(i):
        for cp in yx[i]:
            cp.wait_recv()
        start(cc[i][3:])

    def st_done(i):
        for cp in cc[i]:
            cp.wait_recv()
        for cp in (*zc[i], *xy[i], *yx[i], *cc[i]):
            cp.wait_send()

    def tick(k):
        if 0 <= k < len(msgs):
            st_xy(k)
        if 0 <= k - 1 < len(msgs):
            st_yx(k - 1)
        if 0 <= k - 2 < len(msgs):
            st_c(k - 2)
        if 0 <= k - 3 < len(msgs):
            st_done(k - 3)

    def own_blocks(l):
        for cp in xc[l]:
            cp.wait()
        for j in range(2):
            pieces = XR[:, 2 * l + j].reshape(GROUP * PAD, D)
            W[3 * l + j, b, c] = dot(pick, pieces, NN).astype(BF)

    st_z(0)
    start(xc[0])
    st_z(1)
    XR[q] = XS[q]
    own_blocks(0)
    for i in (2, 3, 4):
        st_z(i)
    start(xc[1])

    def sigmoid(t):
        return 0.5 * jnp.tanh(0.5 * t) + 0.5

    halves = 2
    ht = mt // halves

    def sub_tile(i, k):
        return pl.ds(aligned(i * mt + k * ht, ht), ht)

    def row_tile(i):
        return pl.ds(aligned(i * mt, mt), mt)

    def norm_all(src, with_a, with_t):
        @pl.loop(0, tiles)
        def _(i):
            rows = row_tile(i)
            wide = src[rows, :].astype(F32)
            scale = lax.rsqrt(jnp.mean(wide * wide, -1, keepdims=True) + 1e-6)
            v = (wide * scale).astype(BF)
            if with_a:
                a[rows, :] = v
            if with_t:
                aT[:, rows] = v.T
                ctT[:, rows] = ct[rows, :].T
            acc[rows, :] = jnp.zeros((mt, D), F32)

    def lanes(s):
        return pl.ds(aligned(s * LN, LN), LN)

    def columns(m, s):
        cols = []
        for q in range(4):
            cols.append(jnp.concatenate([W[m, 2 * g + q // 2, q % 2, :, lanes(s)] for g in range(8)], axis=0))
        return jnp.concatenate(cols, axis=1)

    def down_places(s):
        at_t = []
        for t in range(8):
            j = 8 * s + t
            k = lax.div(j, 5)
            at_t.append((lax.div(k, 2), lax.rem(k, 2), pl.ds(pl.multiple_of(lax.rem(j, 5) * 16, 16), 16)))
        return [[(4 * q_ + b_, c_, r_) for b_, c_, r_ in at_t] for q_ in range(4)]

    def down_rows(m, s):
        return jnp.concatenate([W[m, b_, c_, r_, :] for by_t in down_places(s) for b_, c_, r_ in by_t], axis=0)

    def keep(l, n):
        return pltpu.make_async_copy(G.at[n % 2], gu_hbm.at[l, n], gsem.at[n % 2])

    def fetch(n):
        if isinstance(n, int):
            return pltpu.make_async_copy(gu_hbm.at[1 - n // (CH * tiles), n % (CH * tiles)], G.at[n % 2], gsem.at[n % 2])
        return pltpu.make_async_copy(gu_hbm.at[1 - lax.div(n, CH * tiles), lax.rem(n, CH * tiles)], G.at[lax.rem(n, 2)], gsem.at[lax.rem(n, 2)])

    def keep_act(s):
        return pltpu.make_async_copy(E.at[s % 2], act_hbm.at[s], esem.at[s % 2])

    def fetch_act(s):
        return pltpu.make_async_copy(act_hbm.at[s], E.at[s % 2], esem.at[s % 2])

    def forward_tile(l, s, i, n):
        @pl.when(n >= 2)
        def _():
            keep(l, n - 2).wait()

        wgc = columns(3 * l, s)
        wuc = columns(3 * l + 1, s)
        gu_ = []
        for k in range(halves):
            v = a[sub_tile(i, k), :]
            gu_.append((dot(v, wgc, NN), dot(v, wuc, NN)))
        for k, (g, u) in enumerate(gu_):
            G[lax.rem(n, 2), 0, k * ht:(k + 1) * ht, :] = g
            G[lax.rem(n, 2), 1, k * ht:(k + 1) * ht, :] = u
            act = (g * sigmoid(g) * u).astype(BF)
            E[s % 2, sub_tile(i, k), :] = act
            if l == 0:
                acc[sub_tile(i, k), :] += dot(act, down_rows(2, s), NN)
        keep(l, n).start()

    def down_grad(k):
        r = dot(ctT[...], E[k % 2], NN).astype(BF).T
        for qq, by_t in enumerate(down_places(k)):
            for t, (b_, c_, r_) in enumerate(by_t):
                TD[0, b_, c_, r_, :] = r[LN * qq + 16 * t:LN * qq + 16 * (t + 1), :]

    def back_tile(m, s, i, n):
        fetch(n).wait()

        @pl.when(n + 1 < 2 * CH * tiles)
        def _():
            fetch(n + 1).start()

        wgc = columns(m, s)
        wuc = columns(m + 1, s)
        wdr = down_rows(m + 2, s)
        both = jnp.concatenate([wgc, wuc], axis=1)
        dacts = [dot(ct[sub_tile(i, k), :], wdr, NT) for k in range(halves)]
        for k in range(halves):
            dact = dacts[k].astype(BF).astype(F32)
            g = G[lax.rem(n, 2), 0, k * ht:(k + 1) * ht, :]
            u = G[lax.rem(n, 2), 1, k * ht:(k + 1) * ht, :]
            sg = sigmoid(g)
            si = g * sg
            du = (dact * si).astype(BF)
            dg = (dact * u * (sg + si * (1 - sg))).astype(BF)
            E[0, sub_tile(i, k), :] = dg
            E[1, sub_tile(i, k), :] = du
            acc[sub_tile(i, k), :] += dot(jnp.concatenate([dg, du], axis=1), both, NT)

    def back_weights(m, s):
        for j in range(2):
            r = dot(aT[...], E[j], NN).astype(BF)
            for qq in range(4):
                for g in range(8):
                    W[m + j, 2 * g + qq // 2, qq % 2, :, lanes(s)] = r[ROWS * g:ROWS * (g + 1), LN * qq:LN * (qq + 1)]

    def back_norm(src):
        @pl.loop(0, tiles)
        def _(i):
            rows = row_tile(i)
            wide = src[rows, :].astype(F32)
            scale = lax.rsqrt(jnp.mean(wide * wide, -1, keepdims=True) + 1e-6)
            da = acc[rows, :].astype(BF).astype(F32)
            inner = jnp.mean(da * wide, -1, keepdims=True)
            dh = (da * scale - wide * (scale * scale * scale * inner)).astype(BF)
            ct[rows, :] = (ct[rows, :].astype(F32) + dh.astype(F32)).astype(BF)

    class Reduce:
        def __init__(self, term, m, n, ln, slot, bufs, ss, rr):
            self.term, self.m, self.n, self.ln = term, m, n, ln
            self.r1, self.r2, self.r3, self.r4, self.s2, self.s3, self.s4 = bufs
            self.slot = slot
            self.c1 = rcopy(term.at[pl.ds(m, n), :, nc, :, ln], self.r1.at[slot], d_core, ss.at[slot, 0], rr.at[slot, 0])
            self.c2 = [rcopy(self.s2[k], self.r2.at[slot, k], (d_y, d_x)[k], ss.at[slot, 1 + k], rr.at[slot, 1 + k]) for k in (0, 1)]
            self.c3 = [rcopy(self.s3[k], self.r3.at[slot, k], (d_x, d_y)[k], ss.at[slot, 3 + k], rr.at[slot, 3 + k]) for k in (0, 1)]
            self.c4 = [rcopy(self.s4[k], self.r4.at[slot, k], d_z[k], ss.at[slot, 5 + k], rr.at[slot, 5 + k]) for k in range(3)]

        def two(self, j, b_):
            return self.term[self.m + j, b_, c, :, self.ln].astype(F32) + self.r1[self.slot, j, b_].astype(F32)

        def send1(self):
            self.c1.start()

        def send2(self):
            self.c1.wait()
            for j in range(self.n):
                for k in range(2):
                    for l in range(2):
                        self.s2[0][j, 2 * k + l] = self.two(j, 8 * k + 4 * ny + l).astype(BF)
                        self.s2[1][j, 2 * k + l] = self.two(j, 8 * nx + 4 * k + 2 + l).astype(BF)
            for cp in self.c2:
                cp.start()

        def send3(self):
            for cp in self.c2:
                cp.wait()
            for j in range(self.n):
                for l in range(2):
                    v = self.two(j, 8 * nx + 4 * y + l) + self.r2[self.slot, 0, j, 2 * nx + l].astype(F32)
                    self.s3[0][j, l] = v.astype(BF)
                    v = self.two(j, 8 * x + 4 * ny + 2 + l) + self.r2[self.slot, 1, j, 2 * ny + l].astype(F32)
                    self.s3[1][j, l] = v.astype(BF)
            for cp in self.c3:
                cp.start()

        def four(self, j, z_):
            h_ = z_ // 2
            l_ = z_ % 2
            v = self.two(j, 8 * x + 4 * y + z_)
            v += self.r2[self.slot, h_, j, 2 * (x * (1 - h_) + y * h_) + l_].astype(F32)
            return v + self.r3[self.slot, h_, j, l_].astype(F32)

        def send4(self):
            for cp in self.c3:
                cp.wait()
            for j in range(self.n):
                for k in range(3):
                    self.s4[k][j] = self.four(j, zs[k]).astype(BF)
            for cp in self.c4:
                cp.start()

        def finish(self, store):
            for cp in self.c4:
                cp.wait()
            for j in range(self.n):
                v = self.four(j, z)
                for k in range(3):
                    v += self.r4[self.slot, k, j].astype(F32)
                store(j, v.astype(BF))

    gu_bufs = (R1, R2, R3, R4, [S2.at[k] for k in range(2)], [S3.at[k] for k in range(2)], [S4.at[k] for k in range(3)])
    d_bufs = (R1d, R2d, R3d, R4d, [TD.at[pl.ds(0, 1), pl.ds(4 * k, 4), nc] for k in range(2)],
              [TD.at[pl.ds(0, 1), pl.ds(8 + 2 * k, 2), nc] for k in range(2)], [TD.at[pl.ds(0, 1), 12 + k, nc] for k in range(3)])

    def layer_of(t):
        return 1 - lax.div(t, CH)

    def gu(t):
        return Reduce(W, 3 * layer_of(t), 2, lanes(lax.rem(t, CH)), lax.rem(t, SLOTS), gu_bufs, rs_s, rs_r)

    down = Reduce(TD, 0, 1, pl.ds(0, D), 0, d_bufs, rd_s, rd_r)

    def store_gu(t):
        l = layer_of(t)

        def f(j, v):
            OB[l, j, :, lanes(lax.rem(t, CH))] = v
        return f

    def store_d(t):
        l = layer_of(t)

        def f(j, v):
            out_d[l] = v
        return f

    def chunk(t, f):
        @pl.when((t >= 0) & (t < 2 * CH))
        def _():
            f(gu(t))

    def yc(l):
        return [rcopy(XS.at[qs[k], pl.ds(2 * l, 2)], XR.at[q, pl.ds(2 * l, 2)], d_q[k], ys_s.at[l, k], ys_r.at[l, k]) for k in range(3)]

    def hand_back(l):
        for j in range(2):
            r = dot(place, OB[l, j], NN).astype(BF)
            for qq in range(GROUP):
                XS[qq, 2 * l + j] = r[PAD * qq:PAD * (qq + 1), :]
        for cp in yc(l):
            cp.start()

    def take_back(l):
        XR[q, pl.ds(2 * l, 2)] = XS[q, pl.ds(2 * l, 2)]
        for cp in yc(l):
            cp.wait()
        for j, o in enumerate((out_g, out_u)):
            for qq in range(GROUP):
                o[l, :, D * qq:D * (qq + 1)] = XR[qq, 2 * l + j, 0:PIECE, :]

    tick(0)
    tick(1)
    own_blocks(1)
    for i in range(5, len(msgs)):
        st_z(i)
    loads[2].wait()
    norm_all(h, True, False)
    tick(2)
    tick(3)
    tick(4)
    tick(5)

    def at(n, k, f):
        @pl.when(n == k)
        def _():
            f()

    def forward_hooks(n):
        def f4():
            st_xy(6)
            st_yx(5)

        def f8():
            st_c(4)
            st_done(3)

        def f12():
            st_xy(7)
            st_yx(6)

        def f16():
            st_c(5)
            st_done(4)

        def f18():
            st_xy(8)
            st_yx(7)

        for k, f in ((4, f4), (8, f8), (12, f12), (16, f16), (18, f18)):
            at(n, k, f)

    @pl.loop(0, CH * tiles)
    def _(n):
        forward_hooks(n)
        s = lax.div(n, tiles)
        i = lax.rem(n, tiles)

        @pl.when((i == 0) & (s >= 2))
        def _():
            keep_act(s - 2).wait()

        forward_tile(0, s, i, n)

        @pl.when(i == tiles - 1)
        def _():
            keep_act(s).start()

    @pl.loop(0, tiles)
    def _(i):
        rows = row_tile(i)
        h[rows, :] = (h[rows, :].astype(F32) + acc[rows, :].astype(BF).astype(F32)).astype(BF)

    st_c(6)
    loads[3].wait()
    norm_all(h, True, True)
    for n in (CH * tiles - 2, CH * tiles - 1):
        keep(0, n).wait()
    for s in (CH - 2, CH - 1):
        keep_act(s).wait()
    st_done(5)

    @pl.loop(0, CH)
    def _(s):
        def f1():
            st_xy(9)
            st_yx(8)
            st_c(7)

        def f2():
            st_done(6)

        def f3():
            st_yx(9)
            st_c(8)

        def f4():
            st_done(7)

        for k, f in ((1, f1), (2, f2), (3, f3), (4, f4)):
            at(s, k, f)

        @pl.loop(0, tiles)
        def _(i):
            forward_tile(1, s, i, s * tiles + i)

        down_grad(s)

    down.send1()
    for n in (CH * tiles - 2, CH * tiles - 1):
        keep(1, n).wait()
    fetch(0).start()
    pltpu.make_async_copy(x_hbm, a, lsem.at[2]).start()
    st_c(9)
    st_done(8)
    st_done(9)

    @pl.loop(0, 2 * CH + 2)
    def _(t):
        m = 3 * (1 - lax.div(t, CH))
        s = lax.rem(t, CH)
        compute = t < 2 * CH

        @pl.when(compute)
        def _():
            @pl.loop(0, tiles)
            def _(i):
                at(i, 2, lambda: chunk(t - 1, lambda r: r.send2()))
                at(i, 3, lambda: chunk(t - 2, lambda r: r.send4()))
                back_tile(m, s, i, t * tiles + i)

            at(s, 0, lambda: down.send2())
            at(s, 1, lambda: down.send3())
            at(s, 2, lambda: down.send4())
            at(s, 3, lambda: down.finish(store_d(t)))
            back_weights(m, s)

        @pl.when(t >= 2 * CH)
        def _():
            chunk(t - 1, lambda r: r.send2())
            chunk(t - 2, lambda r: r.send4())

        chunk(t, lambda r: r.send1())
        chunk(t - 1, lambda r: r.send3())
        chunk(t - 2, lambda r: r.finish(store_gu(t - 2)))

        @pl.when(t == CH - 1)
        def _():
            fetch_act(0).start()
            fetch_act(1).start()
            back_norm(h)
            pltpu.make_async_copy(x_hbm, a, lsem.at[2]).wait()
            norm_all(a, False, True)

            @pl.loop(0, CH)
            def _(k):
                fetch_act(k).wait()
                down_grad(k)

                @pl.when(k + 2 < CH)
                def _():
                    fetch_act(k + 2).start()

            down.send1()

        @pl.when(t == CH + 1)
        def _():
            hand_back(1)

        @pl.when(t == 2 * CH - 1)
        def _():
            back_norm(a)
            pltpu.make_async_copy(ct, out_x, lsem.at[3]).start()

    hand_back(0)
    take_back(1)
    take_back(0)
    pltpu.make_async_copy(ct, out_x, lsem.at[3]).wait()


def step(x, dy, wg, wu, wd):
    t = x.shape[1]
    mt = t // TILES
    ag = 16 * 10
    dma = pltpu.SemaphoreType.DMA

    def v(*shape, dtype=BF):
        return pltpu.VMEM(shape, dtype)

    def rs_bufs(slots, n, w):
        r = [v(slots, n, 16, ROWS, w), v(slots, 2, n, 4, ROWS, w), v(slots, 2, n, 2, ROWS, w), v(slots, 3, n, ROWS, w)]
        return r, [v(2, n, 4, ROWS, w), v(2, n, 2, ROWS, w), v(3, n, ROWS, w)]

    gr, gs = rs_bufs(SLOTS, 2, LN)
    dr, _ = rs_bufs(1, 1, D)
    vm = pl.BlockSpec(memory_space=pltpu.VMEM)
    hbm = pl.BlockSpec(memory_space=pl.ANY)
    flops = 17 * 2 * t * D * FF

    def out(*shape, dtype=BF):
        return jax.ShapeDtypeStruct(shape, dtype)

    out_x, out_g, out_u, out_d, _, _ = pl.pallas_call(
        kernel,
        out_shape=(out(t, D), out(LAYERS, PIECE, FF), out(LAYERS, PIECE, FF), out(LAYERS, ROWS, D),
                   out(LAYERS, CH * TILES, 2, mt, FC, dtype=F32), out(CH, t, FC)),
        in_specs=[vm, vm, hbm, hbm, hbm],
        out_specs=(hbm, vm, vm, vm, hbm, hbm),
        scratch_shapes=[
            v(6, 16, 2, ROWS, D), v(t, D), v(t, D), v(t, D), v(D, t), v(D, t), v(t, D, dtype=F32), v(2, t, FC),
            v(2, 2, mt, FC, dtype=F32), v(1, 16, 2, ROWS, D),
            *gr, *gs, *dr,
            v(GROUP, 4, PAD, D), v(GROUP, 4, PAD, D), v(LAYERS, 2, ROWS, D),
            dma((4,)), dma((2,)), dma((2,)), dma((ag,)), dma((ag,)), dma((SLOTS, 8)), dma((SLOTS, 8)), dma((1, 8)), dma((1, 8)),
            dma((LAYERS, 3)), dma((LAYERS, 3)), dma((LAYERS, 3)), dma((LAYERS, 3)),
        ],
        compiler_params=pltpu.CompilerParams(collective_id=0, has_side_effects=True, vmem_limit_bytes=67043328),
        cost_estimate=pl.CostEstimate(flops=flops, bytes_accessed=180_000_000, transcendentals=0),
        name="stack",
    )(wg, wu, wd, x[0], dy[0])
    return out_x[None], out_g, out_u, out_d


def solution(mesh):
    w = P(None, "dp", None)
    t = P(("rep", "dp"), None, None)
    o = P("rep", "dp", None)
    return jax.shard_map(step, mesh=mesh, in_specs=(t, t, w, w, w), out_specs=(t, o, o, o), check_vma=False)
```

```python
import jax
import jax.numpy as jnp
from jax import lax
from jax.experimental import pallas as pl
from jax.experimental.pallas import tpu as pltpu
from jax.sharding import PartitionSpec as P

LAYERS = 2
BF = jnp.bfloat16
F32 = jnp.float32
D = 640
FF = 2560
ROWS = 80
CH = 5
LN = 128
FC = 512
GROUP = 4
PIECE = 20
PAD = 32
PARTS = 8
TILES = 4
SLOTS = 4
NN = ((1,), (0,))
NT = ((1,), (1,))


def aligned(i, n):
    return i if isinstance(i, int) else pl.multiple_of(i, n)


def dot(a, b, dims):
    return lax.dot_general(a, b, (dims, ((), ())), preferred_element_type=F32)


def kernel(wg, wu, wd_hbm, x_hbm, dy_hbm, out_x, out_g, out_u, out_d, gu_hbm, act_hbm,
           W, h, ct, a, aT, ctT, acc, E, G, TD, R1, R2, R3, R4, S2, S3, S4,
           R1d, R2d, R3d, R4d, XS, XR, OB,
           lsem, gsem, esem, ag_s, ag_r, rs_s, rs_r, rd_s, rd_r, xs_s, xs_r, ys_s, ys_r):
    T = x_hbm.shape[0]
    tiles = TILES
    mt = T // tiles
    me = lax.axis_index("dp")
    c = me % 2
    z = (me // 2) % 4
    zl = z % 2
    y = (me // 8) % 2
    x = me // 16
    b = me // 2
    q = me % GROUP
    nc = 1 - c
    nx = 1 - x
    ny = 1 - y

    def dev(x_, y_, z_, c_):
        return {"dp": ((x_ * 2 + y_) * 4 + z_) * 2 + c_}

    d_core = dev(x, y, z, nc)
    d_x = dev(nx, y, z, c)
    d_y = dev(x, ny, z, c)
    zs = [(z + k) % 4 for k in (1, 2, 3)]
    d_z = [dev(x, y, zz, c) for zz in zs]
    qs = [(q + k) % GROUP for k in (1, 2, 3)]
    d_q = [{"dp": me - q + qq} for qq in qs]
    everyone = [d_core, d_x, d_y, *d_z, dev(x, y, z + 1 - 2 * zl, nc)]

    def rcopy(src, dst, d, ss, rr):
        return pltpu.make_async_remote_copy(src_ref=src, dst_ref=dst, send_sem=ss, recv_sem=rr,
                                            device_id=d, device_id_type=pl.DeviceIdType.MESH)

    barrier = pltpu.get_barrier_semaphore()
    for d in everyone:
        pl.semaphore_signal(barrier, inc=1, device_id=d, device_id_type=pl.DeviceIdType.MESH)
    loads = [pltpu.make_async_copy(wd_hbm.at[l], W.at[3 * l + 2, b, c], lsem.at[l]) for l in range(LAYERS)]
    loads.append(pltpu.make_async_copy(x_hbm, h, lsem.at[2]))
    loads.append(pltpu.make_async_copy(dy_hbm, ct, lsem.at[3]))
    for cp in loads:
        cp.start()
    for qq in range(GROUP):
        for l in range(LAYERS):
            for j, w in enumerate((wg, wu)):
                XS[qq, 2 * l + j] = jnp.zeros((PAD, D), BF)
                XS[qq, 2 * l + j, 0:PIECE, :] = w[l, :, D * qq:D * (qq + 1)]

    loads[0].wait()
    loads[1].wait()
    pl.semaphore_wait(barrier, len(everyone))

    xc = [[rcopy(XS.at[qs[k], pl.ds(2 * l, 2)], XR.at[q, pl.ds(2 * l, 2)], d_q[k], xs_s.at[l, k], xs_r.at[l, k]) for k in range(3)]
          for l in range(LAYERS)]
    row = lax.broadcasted_iota(jnp.int32, (ROWS, GROUP * PAD), 0)
    col = lax.broadcasted_iota(jnp.int32, (ROWS, GROUP * PAD), 1)
    inside = col % PAD
    pick = jnp.where((inside < PIECE) & (inside + PIECE * (col // PAD) == row), 1.0, 0.0).astype(BF)
    row = lax.broadcasted_iota(jnp.int32, (GROUP * PAD, ROWS), 1)
    col = lax.broadcasted_iota(jnp.int32, (GROUP * PAD, ROWS), 0)
    inside = col % PAD
    place = jnp.where((inside < PIECE) & (inside + PIECE * (col // PAD) == row), 1.0, 0.0).astype(BF)

    msgs = [(2, 1, 0, 128), (2, 1, 128, 512), (0, 2, 0, 256), (0, 2, 256, 256), (0, 2, 512, 128),
            (3, 2, 0, 256), (3, 2, 256, 256), (3, 2, 512, 128), (5, 1, 0, 384), (5, 1, 384, 256)]
    used = [0]

    def part(msg, first, n):
        m, k, lo, w = msg
        return W.at[pl.ds(m, k), pl.ds(first, n), c, :, pl.ds(lo, w)]

    def push(msg, first, n, d):
        i = used[0]
        used[0] += 1
        ref = part(msg, first, n)
        return rcopy(ref, ref, d, ag_s.at[i], ag_r.at[i])

    def start(copies):
        for cp in copies:
            cp.start()

    zc, xy, yx, cc = [], [], [], []
    base = 8 * x + 4 * y
    for g in msgs:
        zc.append([push(g, b, 1, d) for d in d_z])
        xy.append([push(g, base, 2, d_x), push(g, base + 2, 2, d_y)])
        xs2, ys2 = (lambda y_: (4 * y_, 8 + 4 * y_)), (lambda x_: (8 * x_ + 2, 8 * x_ + 6))
        yx.append([push(g, f, 2, d_y) for f in xs2(y)] + [push(g, f, 2, d_x) for f in ys2(x)])
        late = [8 * nx + 4 * y, 8 * x + 4 * ny + 2, *xs2(ny), *ys2(nx)]
        cc.append([push(g, base, 4, d_core)] + [push(g, f, 2, d_core) for f in late])

    def st_z(i):
        start(zc[i])

    def st_xy(i):
        for cp in zc[i]:
            cp.wait_recv()
        start(xy[i])
        start(cc[i][:1])

    def st_yx(i):
        for cp in xy[i]:
            cp.wait_recv()
        start(yx[i])
        start(cc[i][1:3])

    def st_c(i):
        for cp in yx[i]:
            cp.wait_recv()
        start(cc[i][3:])

    def st_done(i):
        for cp in cc[i]:
            cp.wait_recv()
        for cp in (*zc[i], *xy[i], *yx[i], *cc[i]):
            cp.wait_send()

    def tick(k):
        if 0 <= k < len(msgs):
            st_xy(k)
        if 0 <= k - 1 < len(msgs):
            st_yx(k - 1)
        if 0 <= k - 2 < len(msgs):
            st_c(k - 2)
        if 0 <= k - 3 < len(msgs):
            st_done(k - 3)

    def own_blocks(l):
        for cp in xc[l]:
            cp.wait()
        for j in range(2):
            pieces = XR[:, 2 * l + j].reshape(GROUP * PAD, D)
            W[3 * l + j, b, c] = dot(pick, pieces, NN).astype(BF)

    st_z(0)
    start(xc[0])
    st_z(1)
    XR[q] = XS[q]
    own_blocks(0)
    for i in (2, 3, 4):
        st_z(i)
    start(xc[1])

    def sigmoid(t):
        return 0.5 * jnp.tanh(0.5 * t) + 0.5

    halves = 2
    ht = mt // halves

    def sub_tile(i, k):
        return pl.ds(aligned(i * mt + k * ht, ht), ht)

    def row_tile(i):
        return pl.ds(aligned(i * mt, mt), mt)

    def norm_all(src, with_a, with_t):
        @pl.loop(0, tiles)
        def _(i):
            rows = row_tile(i)
            wide = src[rows, :].astype(F32)
            scale = lax.rsqrt(jnp.mean(wide * wide, -1, keepdims=True) + 1e-6)
            v = (wide * scale).astype(BF)
            if with_a:
                a[rows, :] = v
            if with_t:
                aT[:, rows] = v.T
                ctT[:, rows] = ct[rows, :].T
            acc[rows, :] = jnp.zeros((mt, D), F32)

    def lanes(s):
        return pl.ds(aligned(s * LN, LN), LN)

    def columns(m, s):
        cols = []
        for q in range(4):
            cols.append(jnp.concatenate([W[m, 2 * g + q // 2, q % 2, :, lanes(s)] for g in range(8)], axis=0))
        return jnp.concatenate(cols, axis=1)

    def down_places(s):
        at_t = []
        for t in range(8):
            j = 8 * s + t
            k = lax.div(j, 5)
            at_t.append((lax.div(k, 2), lax.rem(k, 2), pl.ds(pl.multiple_of(lax.rem(j, 5) * 16, 16), 16)))
        return [[(4 * q_ + b_, c_, r_) for b_, c_, r_ in at_t] for q_ in range(4)]

    def down_rows(m, s):
        return jnp.concatenate([W[m, b_, c_, r_, :] for by_t in down_places(s) for b_, c_, r_ in by_t], axis=0)

    class Several:
        def __init__(self, copies):
            self.copies = copies

        def start(self):
            for cp in self.copies:
                cp.start()

        def wait(self):
            for cp in self.copies:
                cp.wait()

    def div(i, n):
        return i // n if isinstance(i, int) else lax.div(i, n)

    def rem(i, n):
        return i % n if isinstance(i, int) else lax.rem(i, n)

    def pieces_of(l, n, slot, out):
        copies = []
        for k in range(PARTS):
            j, r = k // (PARTS // 2), pl.ds(k % (PARTS // 2) * (mt // (PARTS // 2)), mt // (PARTS // 2))
            here, there = G.at[slot, j, r], gu_hbm.at[l, n, j, r]
            copies.append(pltpu.make_async_copy(here, there, gsem.at[slot, k]) if out else pltpu.make_async_copy(there, here, gsem.at[slot, k]))
        return Several(copies)

    def keep(l, n):
        return pieces_of(l, n, rem(n, 2), True)

    def fetch(n):
        return pieces_of(1 - div(n, CH * tiles), rem(n, CH * tiles), rem(n, 2), False)

    def keep_act(s):
        return pltpu.make_async_copy(E.at[s % 2], act_hbm.at[s], esem.at[s % 2])

    def fetch_act(s):
        return pltpu.make_async_copy(act_hbm.at[s], E.at[s % 2], esem.at[s % 2])

    def forward_tile(l, s, i, n):
        @pl.when(n >= 2)
        def _():
            keep(l, n - 2).wait()

        wgc = columns(3 * l, s)
        wuc = columns(3 * l + 1, s)
        gu_ = []
        for k in range(halves):
            v = a[sub_tile(i, k), :]
            gu_.append((dot(v, wgc, NN), dot(v, wuc, NN)))
        for k, (g, u) in enumerate(gu_):
            G[lax.rem(n, 2), 0, k * ht:(k + 1) * ht, :] = g
            G[lax.rem(n, 2), 1, k * ht:(k + 1) * ht, :] = u
            act = (g * sigmoid(g) * u).astype(BF)
            E[s % 2, sub_tile(i, k), :] = act
            if l == 0:
                acc[sub_tile(i, k), :] += dot(act, down_rows(2, s), NN)
        keep(l, n).start()

    def down_grad(k):
        r = dot(ctT[...], E[k % 2], NN).astype(BF).T
        for qq, by_t in enumerate(down_places(k)):
            for t, (b_, c_, r_) in enumerate(by_t):
                TD[0, b_, c_, r_, :] = r[LN * qq + 16 * t:LN * qq + 16 * (t + 1), :]

    def back_tile(m, s, i, n):
        fetch(n).wait()

        @pl.when(n + 1 < 2 * CH * tiles)
        def _():
            fetch(n + 1).start()

        wgc = columns(m, s)
        wuc = columns(m + 1, s)
        wdr = down_rows(m + 2, s)
        both = jnp.concatenate([wgc, wuc], axis=1)
        dacts = [dot(ct[sub_tile(i, k), :], wdr, NT) for k in range(halves)]
        for k in range(halves):
            dact = dacts[k].astype(BF).astype(F32)
            g = G[lax.rem(n, 2), 0, k * ht:(k + 1) * ht, :]
            u = G[lax.rem(n, 2), 1, k * ht:(k + 1) * ht, :]
            sg = sigmoid(g)
            si = g * sg
            du = (dact * si).astype(BF)
            dg = (dact * u * (sg + si * (1 - sg))).astype(BF)
            E[0, sub_tile(i, k), :] = dg
            E[1, sub_tile(i, k), :] = du
            acc[sub_tile(i, k), :] += dot(jnp.concatenate([dg, du], axis=1), both, NT)

    def back_weights(m, s):
        for j in range(2):
            r = dot(aT[...], E[j], NN).astype(BF)
            for qq in range(4):
                for g in range(8):
                    W[m + j, 2 * g + qq // 2, qq % 2, :, lanes(s)] = r[ROWS * g:ROWS * (g + 1), LN * qq:LN * (qq + 1)]

    def back_norm(src):
        @pl.loop(0, tiles)
        def _(i):
            rows = row_tile(i)
            wide = src[rows, :].astype(F32)
            scale = lax.rsqrt(jnp.mean(wide * wide, -1, keepdims=True) + 1e-6)
            da = acc[rows, :].astype(BF).astype(F32)
            inner = jnp.mean(da * wide, -1, keepdims=True)
            dh = (da * scale - wide * (scale * scale * scale * inner)).astype(BF)
            ct[rows, :] = (ct[rows, :].astype(F32) + dh.astype(F32)).astype(BF)

    class Reduce:
        def __init__(self, term, m, n, ln, slot, bufs, ss, rr):
            self.term, self.m, self.n, self.ln = term, m, n, ln
            self.r1, self.r2, self.r3, self.r4, self.s2, self.s3, self.s4 = bufs
            self.slot = slot
            self.c1 = rcopy(term.at[pl.ds(m, n), :, nc, :, ln], self.r1.at[slot], d_core, ss.at[slot, 0], rr.at[slot, 0])
            self.c2 = [rcopy(self.s2[k], self.r2.at[slot, k], (d_y, d_x)[k], ss.at[slot, 1 + k], rr.at[slot, 1 + k]) for k in (0, 1)]
            self.c3 = [rcopy(self.s3[k], self.r3.at[slot, k], (d_x, d_y)[k], ss.at[slot, 3 + k], rr.at[slot, 3 + k]) for k in (0, 1)]
            self.c4 = [rcopy(self.s4[k], self.r4.at[slot, k], d_z[k], ss.at[slot, 5 + k], rr.at[slot, 5 + k]) for k in range(3)]

        def two(self, j, b_):
            return self.term[self.m + j, b_, c, :, self.ln].astype(F32) + self.r1[self.slot, j, b_].astype(F32)

        def send1(self):
            self.c1.start()

        def send2(self):
            self.c1.wait()
            for j in range(self.n):
                for k in range(2):
                    for l in range(2):
                        self.s2[0][j, 2 * k + l] = self.two(j, 8 * k + 4 * ny + l).astype(BF)
                        self.s2[1][j, 2 * k + l] = self.two(j, 8 * nx + 4 * k + 2 + l).astype(BF)
            for cp in self.c2:
                cp.start()

        def send3(self):
            for cp in self.c2:
                cp.wait()
            for j in range(self.n):
                for l in range(2):
                    v = self.two(j, 8 * nx + 4 * y + l) + self.r2[self.slot, 0, j, 2 * nx + l].astype(F32)
                    self.s3[0][j, l] = v.astype(BF)
                    v = self.two(j, 8 * x + 4 * ny + 2 + l) + self.r2[self.slot, 1, j, 2 * ny + l].astype(F32)
                    self.s3[1][j, l] = v.astype(BF)
            for cp in self.c3:
                cp.start()

        def four(self, j, z_):
            h_ = z_ // 2
            l_ = z_ % 2
            v = self.two(j, 8 * x + 4 * y + z_)
            v += self.r2[self.slot, h_, j, 2 * (x * (1 - h_) + y * h_) + l_].astype(F32)
            return v + self.r3[self.slot, h_, j, l_].astype(F32)

        def send4(self):
            for cp in self.c3:
                cp.wait()
            for j in range(self.n):
                for k in range(3):
                    self.s4[k][j] = self.four(j, zs[k]).astype(BF)
            for cp in self.c4:
                cp.start()

        def finish(self, store):
            for cp in self.c4:
                cp.wait()
            for j in range(self.n):
                v = self.four(j, z)
                for k in range(3):
                    v += self.r4[self.slot, k, j].astype(F32)
                store(j, v.astype(BF))

    gu_bufs = (R1, R2, R3, R4, [S2.at[k] for k in range(2)], [S3.at[k] for k in range(2)], [S4.at[k] for k in range(3)])
    d_bufs = (R1d, R2d, R3d, R4d, [TD.at[pl.ds(0, 1), pl.ds(4 * k, 4), nc] for k in range(2)],
              [TD.at[pl.ds(0, 1), pl.ds(8 + 2 * k, 2), nc] for k in range(2)], [TD.at[pl.ds(0, 1), 12 + k, nc] for k in range(3)])

    def layer_of(t):
        return 1 - lax.div(t, CH)

    def gu(t):
        return Reduce(W, 3 * layer_of(t), 2, lanes(lax.rem(t, CH)), lax.rem(t, SLOTS), gu_bufs, rs_s, rs_r)

    down = Reduce(TD, 0, 1, pl.ds(0, D), 0, d_bufs, rd_s, rd_r)

    def store_gu(t):
        l = layer_of(t)

        def f(j, v):
            OB[l, j, :, lanes(lax.rem(t, CH))] = v
        return f

    def store_d(t):
        l = layer_of(t)

        def f(j, v):
            out_d[l] = v
        return f

    def chunk(t, f):
        @pl.when((t >= 0) & (t < 2 * CH))
        def _():
            f(gu(t))

    def yc(l):
        return [rcopy(XS.at[qs[k], pl.ds(2 * l, 2)], XR.at[q, pl.ds(2 * l, 2)], d_q[k], ys_s.at[l, k], ys_r.at[l, k]) for k in range(3)]

    def hand_back(l):
        for j in range(2):
            r = dot(place, OB[l, j], NN).astype(BF)
            for qq in range(GROUP):
                XS[qq, 2 * l + j] = r[PAD * qq:PAD * (qq + 1), :]
        for cp in yc(l):
            cp.start()

    def take_back(l):
        XR[q, pl.ds(2 * l, 2)] = XS[q, pl.ds(2 * l, 2)]
        for cp in yc(l):
            cp.wait()
        for j, o in enumerate((out_g, out_u)):
            for qq in range(GROUP):
                o[l, :, D * qq:D * (qq + 1)] = XR[qq, 2 * l + j, 0:PIECE, :]

    tick(0)
    tick(1)
    loads[2].wait()
    norm_all(h, True, False)
    tick(2)
    own_blocks(1)
    for i in range(5, len(msgs)):
        st_z(i)
    tick(3)
    tick(4)
    st_done(2)

    def at(n, k, f):
        @pl.when(n == k)
        def _():
            f()

    def forward_hooks(n):
        for k, calls in (
            (2, ((st_xy, 5), (st_yx, 4))),
            (5, ((st_c, 3),)),
            (8, ((st_done, 3), (st_xy, 6), (st_yx, 5))),
            (11, ((st_c, 4),)),
            (14, ((st_xy, 7), (st_yx, 6))),
            (16, ((st_done, 4),)),
            (17, ((st_c, 5),)),
            (19, ((st_xy, 8), (st_yx, 7))),
        ):
            at(n, k, lambda: [f(i) for f, i in calls] and None)

    @pl.loop(0, CH * tiles)
    def _(n):
        forward_hooks(n)
        s = lax.div(n, tiles)
        i = lax.rem(n, tiles)

        @pl.when((i == 0) & (s >= 2))
        def _():
            keep_act(s - 2).wait()

        forward_tile(0, s, i, n)

        @pl.when(i == tiles - 1)
        def _():
            keep_act(s).start()

    @pl.loop(0, tiles)
    def _(i):
        rows = row_tile(i)
        h[rows, :] = (h[rows, :].astype(F32) + acc[rows, :].astype(BF).astype(F32)).astype(BF)

    st_c(6)
    loads[3].wait()
    norm_all(h, True, True)
    for n in (CH * tiles - 2, CH * tiles - 1):
        keep(0, n).wait()
    for s in (CH - 2, CH - 1):
        keep_act(s).wait()
    st_done(5)

    @pl.loop(0, CH)
    def _(s):
        for k, calls in (
            (1, ((st_xy, 9), (st_yx, 8))),
            (2, ((st_done, 6), (st_c, 7))),
            (3, ((st_yx, 9), (st_c, 8))),
            (4, ((st_done, 7),)),
        ):
            at(s, k, lambda: [f(i) for f, i in calls] and None)

        @pl.loop(0, tiles)
        def _(i):
            forward_tile(1, s, i, s * tiles + i)

        down_grad(s)

    down.send1()
    for n in (CH * tiles - 2, CH * tiles - 1):
        keep(1, n).wait()
    fetch(0).start()
    pltpu.make_async_copy(x_hbm, a, lsem.at[2]).start()
    st_c(9)
    st_done(8)
    st_done(9)

    @pl.loop(0, 2 * CH + 3)
    def _(t):
        m = 3 * (1 - lax.div(t, CH))
        s = lax.rem(t, CH)
        compute = t < 2 * CH

        @pl.when(compute)
        def _():
            @pl.loop(0, tiles)
            def _(i):
                at(i, 1, lambda: chunk(t - 3, lambda r: r.finish(store_gu(t - 3))))
                at(i, 2, lambda: chunk(t - 1, lambda r: r.send2()))
                at(i, 3, lambda: chunk(t - 2, lambda r: r.send4()))
                back_tile(m, s, i, t * tiles + i)

            at(s, 0, lambda: down.send2())
            at(s, 1, lambda: down.send3())
            at(s, 2, lambda: down.send4())
            at(s, 3, lambda: down.finish(store_d(t)))
            back_weights(m, s)

        @pl.when(t >= 2 * CH)
        def _():
            chunk(t - 1, lambda r: r.send2())
            chunk(t - 3, lambda r: r.finish(store_gu(t - 3)))
            chunk(t - 2, lambda r: r.send4())

            @pl.when(t == 2 * CH)
            def _():
                back_norm(a)
                pltpu.make_async_copy(ct, out_x, lsem.at[3]).start()

        chunk(t, lambda r: r.send1())
        chunk(t - 1, lambda r: r.send3())

        @pl.when(t == CH - 1)
        def _():
            fetch_act(0).start()
            fetch_act(1).start()
            back_norm(h)
            pltpu.make_async_copy(x_hbm, a, lsem.at[2]).wait()
            norm_all(a, False, True)

            @pl.loop(0, CH)
            def _(k):
                fetch_act(k).wait()
                down_grad(k)

                @pl.when(k + 2 < CH)
                def _():
                    fetch_act(k + 2).start()

            down.send1()

        @pl.when(t == CH + 2)
        def _():
            hand_back(1)

        @pl.when(t == 2 * CH - 1)
        def _():
            take_back(1)

    hand_back(0)
    take_back(0)
    pltpu.make_async_copy(ct, out_x, lsem.at[3]).wait()


def step(x, dy, wg, wu, wd):
    t = x.shape[1]
    mt = t // TILES
    ag = 16 * 10
    dma = pltpu.SemaphoreType.DMA

    def v(*shape, dtype=BF):
        return pltpu.VMEM(shape, dtype)

    def rs_bufs(slots, n, w):
        r = [v(slots, n, 16, ROWS, w), v(slots, 2, n, 4, ROWS, w), v(slots, 2, n, 2, ROWS, w), v(slots, 3, n, ROWS, w)]
        return r, [v(2, n, 4, ROWS, w), v(2, n, 2, ROWS, w), v(3, n, ROWS, w)]

    gr, gs = rs_bufs(SLOTS, 2, LN)
    dr, _ = rs_bufs(1, 1, D)
    vm = pl.BlockSpec(memory_space=pltpu.VMEM)
    hbm = pl.BlockSpec(memory_space=pl.ANY)
    flops = 17 * 2 * t * D * FF

    def out(*shape, dtype=BF):
        return jax.ShapeDtypeStruct(shape, dtype)

    out_x, out_g, out_u, out_d, _, _ = pl.pallas_call(
        kernel,
        out_shape=(out(t, D), out(LAYERS, PIECE, FF), out(LAYERS, PIECE, FF), out(LAYERS, ROWS, D),
                   out(LAYERS, CH * TILES, 2, mt, FC, dtype=F32), out(CH, t, FC)),
        in_specs=[vm, vm, hbm, hbm, hbm],
        out_specs=(hbm, vm, vm, vm, hbm, hbm),
        scratch_shapes=[
            v(6, 16, 2, ROWS, D), v(t, D), v(t, D), v(t, D), v(D, t), v(D, t), v(t, D, dtype=F32), v(2, t, FC),
            v(2, 2, mt, FC, dtype=F32), v(1, 16, 2, ROWS, D),
            *gr, *gs, *dr,
            v(GROUP, 4, PAD, D), v(GROUP, 4, PAD, D), v(LAYERS, 2, ROWS, D),
            dma((4,)), dma((2, PARTS)), dma((2,)), dma((ag,)), dma((ag,)), dma((SLOTS, 8)), dma((SLOTS, 8)), dma((1, 8)), dma((1, 8)),
            dma((LAYERS, 3)), dma((LAYERS, 3)), dma((LAYERS, 3)), dma((LAYERS, 3)),
        ],
        compiler_params=pltpu.CompilerParams(collective_id=0, has_side_effects=True, vmem_limit_bytes=67043328),
        cost_estimate=pl.CostEstimate(flops=flops, bytes_accessed=180_000_000, transcendentals=0),
        name="stack",
    )(wg, wu, wd, x[0], dy[0])
    return out_x[None], out_g, out_u, out_d


def solution(mesh):
    w = P(None, "dp", None)
    t = P(("rep", "dp"), None, None)
    o = P("rep", "dp", None)
    return jax.shard_map(step, mesh=mesh, in_specs=(t, t, w, w, w), out_specs=(t, o, o, o), check_vma=False)
```
